32 devices in a mesh: dp: 8 (over y, x, core), tensor: 4 (over z).
Axes of the slice: x: 2, y: 2, z: 4, core: 2. Of those that a mesh axis runs over, the one named last changes fastest.
Arguments:
- tokens: bfloat16 [128, 8192], P('dp'), may hold values from -6 to 6
- norm_gain: bfloat16 [8192], replicated, may hold values from 0.099609375 to 1.8984375
- w_query: bfloat16 [8192, 8192], P('dp', 'tensor'), may hold values from -0.0625 to 0.0625
- w_key: bfloat16 [8192, 1024], P('dp', 'tensor'), may hold values from -0.0625 to 0.0625
- w_value: bfloat16 [8192, 1024], P('dp', 'tensor'), may hold values from -0.0625 to 0.0625
- check_column: bfloat16 [8192], replicated, may hold values from -6 to 6
- key_cache: bfloat16 [4096, 16, 8, 128], P('dp', None, 'tensor'), may hold values from -320 to 320
- value_cache: bfloat16 [4096, 16, 8, 128], P('dp', None, 'tensor'), may hold values from -6 to 6
- page_table: int32 [128, 32], P('dp'), may hold values from 0 to 511, as said below
- lengths: int32 [128], P('dp'), may hold values from 1 to 512, as said below
- tol_counts: int32 [128], replicated, may hold values from 0 to 7
Outputs:
- attention: bfloat16 [128, 8192], P('dp', 'tensor')
- excess: float32 [], replicated
The draws below stay inside these ranges and needn't reach their ends.
Inputs may be any that keep to these rules, and one draw needn't show every extreme that they name: page_table holds pool pages of the index of dp that holds the sequence; the 16 sequences of one index of dp own distinct pages and together own all 512 of them. `lengths`: some sequence holds exactly 512 cached tokens.
All inputs are finite; a program needn't handle non-finite values.
Results may differ from the reference program's by a relative error of at most 0.007.
The reference program's roundings to bfloat16 on the way count: a program that leaves them out, or rounds other values in their place, can miss the bound.
Values may be sent and summed in bfloat16 or wider, within the bound.
A program may use at most 64 MiB of HBM per device.

```python
import jax
import jax.numpy as jnp
from jax import lax

D = 8192
HQ = 64
KVH = 8
HD = 128
SEQ_DEV = 16
MAXP = 32
PAGE = 16
CTX = 512
POOL = 512
PAGES_ALL = 4096
B = 128


def draw_page_table(key, part):
    subkeys = jax.random.split(key, B // SEQ_DEV)

    def one_order(subkey):
        return jax.random.permutation(subkey, SEQ_DEV * MAXP)
    orders = jax.vmap(one_order)(subkeys)
    return orders.reshape(B, MAXP).astype(jnp.int32)


def draw_lengths(key, part):
    drawn = jax.random.randint(jax.random.fold_in(key, 3), (B,), 1, CTX + 1)
    return drawn.at[0].set(CTX).astype(jnp.int32)


def draw_key_cache(key, part):
    normal_part = jax.random.truncated_normal(jax.random.fold_in(key, 5), -4.0, 4.0, (PAGES_ALL, PAGE, KVH, HD), jnp.float32)
    return (normal_part * 2.2).astype(jnp.bfloat16)


def set_ends(result, own_key, low, high):
    longest = result.shape.index(max(result.shape))
    spots = []
    for shift in (0, 1):
        where = [jax.random.randint(jax.random.fold_in(own_key, axis), (), 0, length) for axis, length in enumerate(result.shape)]
        where[longest] = (where[longest] + shift) % result.shape[longest]
        spots.append(tuple(where))
    return result.at[spots[0]].set(low).at[spots[1]].set(high)


def block_scale(rng, shape, cuts, smallest, top_value):
    def one(position, blocks):
        steps = jax.random.uniform(jax.random.fold_in(jax.random.fold_in(rng, 6), position), (blocks,), jnp.float32, smallest / len(cuts), top_value / len(cuts))
        return jnp.repeat(jnp.exp(steps), shape[position] // blocks).reshape((-1,) + (1,) * (len(shape) - position - 1))

    loudness = one(*cuts[0])
    for cut in cuts[1:]:
        loudness = loudness * one(*cut)
    return loudness


def gaussian(rng, extent, spread, most, cuts=(), kind=jnp.bfloat16):
    result = jax.random.normal(rng, extent, jnp.float32) * spread
    if len(cuts) > 0:
        result = block_scale(rng, extent, cuts, -0.22, 0.18) * result
    return jnp.clip(result, min=-most, max=most).astype(kind)


def setup_inputs(seed: int = 0) -> dict:
    splits = jax.random.split(jax.random.key(seed), 12)
    tokens = gaussian(splits[0], (B, D), 1.0, 6.0, ((0, 8),))
    norm_gain = jnp.clip(1.0 + 0.18 * jax.random.normal(splits[1], (D,), jnp.float32), 0.099609375, 1.8984375).astype(jnp.bfloat16)
    w_query = gaussian(splits[2], (D, HQ * HD), D ** -0.5, 0.0625, ((0, 8), (1, 4)))
    w_key = gaussian(splits[3], (D, KVH * HD), D ** -0.5, 0.0625, ((0, 8), (1, 4)))
    w_value = gaussian(splits[4], (D, KVH * HD), D ** -0.5, 0.0625, ((0, 8), (1, 4)))
    check_column = gaussian(splits[5], (D,), (((HQ + 2 * KVH) * HD / D) ** 0.5), 6.0)
    key_cache = draw_key_cache(jax.random.fold_in(splits[11], 71), 0)
    value_cache = gaussian(splits[7], (PAGES_ALL, PAGE, KVH, HD), 1.0, 6.0, ((0, 8), (2, 4)))
    page_table = draw_page_table(jax.random.fold_in(splits[11], 71), 0)
    lengths = draw_lengths(jax.random.fold_in(splits[11], 71), 0)
    tol_counts = set_ends(jax.random.randint(splits[10], (B,), 0, 8), jax.random.fold_in(splits[10], 1), 0, 7).astype(jnp.int32)
    return {"tokens": tokens, "norm_gain": norm_gain, "w_query": w_query, "w_key": w_key, "w_value": w_value, "check_column": check_column, "key_cache": key_cache, "value_cache": value_cache, "page_table": page_table, "lengths": lengths, "tol_counts": tol_counts}


epsilon = 1e-06
rope_base = 1000000.0
tol_step = 0.25

def normalize(tokens, norm_gain):
    widened = tokens.astype(jnp.float32)
    mean_square = lax.optimization_barrier(jnp.mean(widened * widened, axis=1, keepdims=True))
    return (widened * lax.rsqrt(mean_square + epsilon) * norm_gain.astype(jnp.float32)).astype(jnp.bfloat16)

def rotate(vectors, positions):
    half_width = vectors.shape[-1] // 2
    steps_index = jnp.arange(half_width, dtype=jnp.float32)
    inverse = rope_base ** (-2.0 * steps_index / vectors.shape[-1])
    angles = positions.astype(jnp.float32)[:, None] * inverse[None, :]
    cosine = jnp.cos(angles)[:, None, :]
    sine_part = jnp.sin(angles)[:, None, :]
    lower = vectors[..., :half_width]
    upper = vectors[..., half_width:]
    return jnp.concatenate([lower * cosine - upper * sine_part, upper * cosine + lower * sine_part], axis=-1)

def attend(query_heads, cached_keys, cached_values, key_new, value_new, lengths):
    score_scale = query_heads.shape[-1] ** (-0.5)
    query_wide = query_heads.astype(jnp.float32)
    scores = jnp.einsum('skgd,sckd->skgc', query_wide, cached_keys.astype(jnp.float32)) * score_scale
    new_score = jnp.einsum('skgd,skd->skg', query_wide, key_new.astype(jnp.float32)) * score_scale
    live_mask = (jnp.arange(cached_keys.shape[1])[None, :] < lengths[:, None])[:, None, None, :]
    masked = jnp.where(live_mask, scores, -jnp.inf)
    peak_score = jnp.maximum(lax.optimization_barrier(jnp.max(masked, axis=-1)), new_score)
    weights = jnp.exp(masked - peak_score[..., None])
    new_weight = jnp.exp(new_score - peak_score)
    denominator = lax.optimization_barrier(jnp.sum(weights, axis=-1)) + new_weight
    rounded = lax.optimization_barrier(weights.astype(jnp.bfloat16)).astype(jnp.float32)
    rounded_new = lax.optimization_barrier(new_weight.astype(jnp.bfloat16)).astype(jnp.float32)
    mixed_heads = jnp.einsum('skgc,sckd->skgd', rounded, cached_values.astype(jnp.float32))
    mixed_heads = mixed_heads + rounded_new[..., None] * value_new.astype(jnp.float32)[:, :, None, :]
    return mixed_heads / denominator[..., None]

def reference(tokens, norm_gain, w_query, w_key, w_value, check_column, key_cache, value_cache, page_table, lengths, tol_counts):
    normed = normalize(tokens, norm_gain)
    query_all = jnp.dot(normed, w_query, preferred_element_type=jnp.float32)
    key_all = jnp.dot(normed, w_key, preferred_element_type=jnp.float32)
    value_all = jnp.dot(normed, w_value, preferred_element_type=jnp.float32)
    column_count = query_all.shape[1] + key_all.shape[1] + value_all.shape[1]
    row_sums = lax.optimization_barrier(jnp.sum(query_all, axis=1)) + lax.optimization_barrier(jnp.sum(key_all, axis=1)) + lax.optimization_barrier(jnp.sum(value_all, axis=1))
    check_sums = jnp.dot(normed, check_column, preferred_element_type=jnp.float32)
    residual = (row_sums - check_sums) / jnp.sqrt(jnp.float32(column_count))
    token_excess = jnp.maximum(jnp.abs(residual) - tol_step * tol_counts.astype(jnp.float32), 0.0)
    excess = jnp.sum(token_excess) / jnp.sqrt(jnp.float32(B))
    query_heads = rotate(query_all.reshape(B, HQ, HD), lengths).astype(jnp.bfloat16)
    key_new = rotate(key_all.reshape(B, KVH, HD), lengths).astype(jnp.bfloat16)
    value_new = value_all.reshape(B, KVH, HD).astype(jnp.bfloat16)
    owner_base = (jnp.arange(B) // SEQ_DEV * POOL).astype(jnp.int32)
    global_pages = (page_table + owner_base[:, None]).astype(jnp.int32)

    def one_sequence(inputs):
        query_one, key_one, value_one, pages_one, length_one = inputs
        cached_keys = key_cache[pages_one].reshape(1, CTX, KVH, HD)
        cached_values = value_cache[pages_one].reshape(1, CTX, KVH, HD)
        mixed_heads = attend(query_one.reshape(1, KVH, HQ // KVH, HD), cached_keys, cached_values, key_one[None], value_one[None], length_one[None])
        return mixed_heads.reshape(HQ * HD).astype(jnp.bfloat16)
    attention = lax.map(one_sequence, (query_heads, key_new, value_new, global_pages, lengths))
    return (attention, excess)
```

```python
import functools
import math

import jax
import jax.numpy as jnp
from jax import lax
from jax.experimental import pallas as pl
from jax.experimental.pallas import tpu as pltpu
from jax.sharding import PartitionSpec as P

EPSILON = 1e-06
ROPE_BASE = 1000000.0
TOL_STEP = 0.25
MESH = pl.DeviceIdType.MESH
F32 = jnp.float32
BF16 = jnp.bfloat16
UNROLL = 4
LANES = 128


def step_kernel(
    dp,
    tp,
    table_hbm,
    lengths_hbm,
    counts_hbm,
    tokens_hbm,
    gain_hbm,
    check_hbm,
    wq_hbm,
    wk_hbm,
    wv_hbm,
    keys_hbm,
    values_hbm,
    out_ref,
    excess_ref,
    table_ref,
    lengths_ref,
    counts_ref,
    tokens_ref,
    gain_ref,
    check_ref,
    weights,
    keys,
    values,
    key_columns,
    outgoing,
    spread,
    parts,
    from_pair,
    from_chips,
    queries,
    new_keys,
    new_values,
    mixed,
    sums_all,
    sums_own,
    shares,
    excess_all,
    excess_own,
    small_sems,
    load_sems,
    a2a_send,
    a2a_recv,
    pair_send,
    pair_recv,
    chip_send,
    chip_recv,
    sum_send,
    sum_recv,
    exc_send,
    exc_recv,
):
    chips = dp // 2
    me = lax.axis_index("dp")
    zed = lax.axis_index("tensor")
    chip, core = me // 2, me % 2
    seqs, width = tokens_ref.shape
    depth = width // dp
    q_width, kv_width = wq_hbm.shape[1], wk_hbm.shape[1]
    total = q_width + 2 * kv_width
    chunks, _, _, chunk = parts.shape
    head = keys_hbm.shape[2]
    q_heads, kv_heads = q_width // head, kv_width // head
    group = q_heads // kv_heads
    pages = table_ref.shape[1]
    page_rows = keys_hbm.shape[1]

    def partner(dc):
        other, bit = chip, 1
        while bit <= dc:
            if dc // bit % 2:
                other = other + bit - 2 * bit * (chip // bit % 2)
            bit *= 2
        return other

    barrier = pltpu.get_barrier_semaphore()
    for k in range(1, dp):
        pl.semaphore_signal(
            barrier, inc=1, device_id=((me + k) % dp, zed), device_id_type=MESH
        )

    small_loads = [
        pltpu.make_async_copy(source, target, small_sems.at[i])
        for i, (source, target) in enumerate(
            [
                (tokens_hbm, tokens_ref),
                (gain_hbm, gain_ref),
                (lengths_hbm, lengths_ref),
                (check_hbm, check_ref),
                (table_hbm, table_ref),
                (counts_hbm, counts_ref),
            ]
        )
    ]
    for load in small_loads:
        load.start()
    loads = [
        pltpu.make_async_copy(wq_hbm, weights.at[:, pl.ds(0, q_width)], load_sems.at[0]),
        pltpu.make_async_copy(wk_hbm, weights.at[:, pl.ds(q_width, kv_width)], load_sems.at[0]),
        pltpu.make_async_copy(
            wv_hbm, weights.at[:, pl.ds(q_width + kv_width, kv_width)], load_sems.at[0]
        ),
        pltpu.make_async_copy(keys_hbm, keys, load_sems.at[1]),
        pltpu.make_async_copy(values_hbm, values, load_sems.at[2]),
    ]
    for load in loads:
        load.start()

    for load in small_loads[:2]:
        load.wait()
    square = jnp.zeros((seqs, LANES), F32)
    for j in range(width // LANES):
        part = tokens_ref[:, j * LANES : (j + 1) * LANES].astype(F32)
        square = square + part * part
    scale = lax.rsqrt(jnp.sum(square, axis=1, keepdims=True) / width + EPSILON)
    gains = gain_ref[...].astype(F32)
    for j in range(width // LANES):
        part = tokens_ref[:, j * LANES : (j + 1) * LANES].astype(F32)
        at = j * LANES % depth
        outgoing[j * LANES // depth, :, at : at + LANES] = (
            part * scale * gains[j : j + 1]
        ).astype(BF16)
    spread[0] = outgoing[me]

    pl.semaphore_wait(barrier, dp - 1 + (zed + tp - 1) // tp)

    def greet_plane(k):
        @pl.when((zed + k >= 0) & (zed + k < tp))
        def _():
            pl.semaphore_signal(barrier, inc=1, device_id=(me, zed + k), device_id_type=MESH)


    for dc in range(chips - 1, -1, -1):
        for q in range(2):
            if dc == 0 and q == 0:
                continue
            target = partner(dc) * 2 + (core + q) % 2
            copy = pltpu.make_async_remote_copy(
                src_ref=outgoing.at[target],
                dst_ref=spread.at[q * chips + dc],
                send_sem=a2a_send,
                recv_sem=a2a_recv,
                device_id=(target, zed),
                device_id_type=MESH,
            )
            copy.start()

    greet_plane(1)
    for k in range(1, tp):
        greet_plane(-k)

    for load in small_loads[2:]:
        load.wait()
    checks = check_ref[...].astype(F32)
    checked = jnp.zeros((seqs, LANES), F32)
    for j in range(width // LANES):
        at = j * LANES % depth
        part = outgoing[j * LANES // depth, :, at : at + LANES].astype(F32)
        checked = checked + part * checks[j : j + 1]

    seq_row = lax.broadcasted_iota(jnp.int32, (seqs, LANES), 0)
    positions = jnp.zeros((seqs, LANES), F32)
    for s in range(seqs):
        positions = jnp.where(seq_row == s, lengths_ref[s].astype(F32), positions)
    lane = lax.broadcasted_iota(jnp.int32, (seqs, head), 1)
    step = (lane % (head // 2)).astype(F32)
    angles = positions * jnp.exp(step * (-2.0 * math.log(ROPE_BASE) / head))
    cosine = jnp.cos(angles)
    sine = jnp.where(lane < head // 2, -1.0, 1.0) * jnp.sin(angles)

    near = (pages + 1) // 2
    far = pages - near
    span = near * page_rows
    no_page = jnp.zeros((page_rows, head), BF16)

    def side_by_side(pool, s):
        left = [pool[table_ref[s, p]] for p in range(near)]
        right = [pool[table_ref[s, p]] for p in range(near, pages)] + [no_page] * (near - far)
        return jnp.concatenate(
            [jnp.concatenate(left, axis=0), jnp.concatenate(right, axis=0)], axis=1
        )

    def turn_keys(s, carry):
        key_columns[s] = jnp.transpose(side_by_side(keys, s))
        return carry

    loads[3].wait()
    lax.fori_loop(0, seqs, turn_keys, 0, unroll=UNROLL)

    def wait_bytes(ref, sem):
        pltpu.make_async_copy(ref, ref, sem).wait()

    wait_bytes(weights, load_sems.at[0])
    wait_bytes(spread.at[pl.ds(1, dp - 1)], a2a_recv)

    pair_copies = []
    half = chips * seqs

    def project(c):
        product = jnp.dot(
            spread[...].reshape(dp * seqs, depth),
            weights[:, pl.ds(c * chunk, chunk)],
            preferred_element_type=F32,
        )
        parts[c, 1] = product[half:]
        copy = pltpu.make_async_remote_copy(
            src_ref=parts.at[c, 1],
            dst_ref=from_pair.at[c],
            send_sem=pair_send,
            recv_sem=pair_recv.at[c],
            device_id=(chip * 2 + (core + 1) % 2, zed),
            device_id_type=MESH,
        )
        copy.start()
        pair_copies.append(copy)
        parts[c, 0] = product[:half]
        return sum(product[:, i : i + LANES] for i in range(0, chunk, LANES))

    def pass_on(c):
        pair_copies[c].wait_recv()
        for dc in range(chips - 1, 0, -1):
            rows = pl.ds(dc * seqs, seqs)
            parts[c, 0, rows] = parts[c, 0, rows] + from_pair[c, rows]
            copy = pltpu.make_async_remote_copy(
                src_ref=parts.at[c, 0, rows],
                dst_ref=from_chips.at[c, dc - 1],
                send_sem=chip_send,
                recv_sem=chip_recv.at[c],
                device_id=(partner(dc) * 2 + core, zed),
                device_id_type=MESH,
            )
            copy.start()

    def exchange(own, everyone, place, targets, send_sem, recv_sem):
        everyone[place] = own[...]
        for target in targets:
            pltpu.make_async_remote_copy(
                src_ref=own,
                dst_ref=everyone.at[place],
                send_sem=send_sem,
                recv_sem=recv_sem,
                device_id=target,
                device_id_type=MESH,
            ).start()

    row_sum = jnp.zeros((dp * seqs, LANES), F32)
    passed = 0
    for c in range(chunks):
        row_sum = row_sum + project(c)
        if c >= 3:
            pass_on(passed)
            passed += 1
    for q in range(2):
        for dc in range(chips):
            owner = partner(dc) * 2 + (core + q) % 2
            at = (q * chips + dc) * seqs
            share = row_sum[at : at + seqs]
            if q == 0 and dc == 0:
                share = share - jnp.where(zed == 0, checked, 0.0)
            shares[owner] = share
    turned_sums = jnp.transpose(shares[...].reshape(dp * seqs, LANES))
    excess_own[...] = jnp.sum(turned_sums, axis=0, keepdims=True)
    exchange(
        excess_own, excess_all, me, [((me + k) % dp, zed) for k in range(1, dp)], exc_send, exc_recv
    )
    while passed < chunks:
        pass_on(passed)
        passed += 1
    wait_bytes(excess_all.at[pl.ds(1, dp - 1)], exc_recv)
    group_sum = excess_all[0]
    for k in range(1, dp):
        group_sum = group_sum + excess_all[k]
    sums_own[...] = group_sum

    @pl.when(zed < tp - 1)
    def _():
        pl.semaphore_wait(barrier, tp - 1 - zed)

    exchange(
        sums_own, sums_all, zed, [(me, (zed + k) % tp) for k in range(1, tp)], sum_send, sum_recv
    )

    def rotate(vector):
        return (
            (vector * cosine + pltpu.roll(vector, head // 2, 1) * sine)
            .astype(BF16)
            .astype(F32)
        )

    for c in range(chunks):
        wait_bytes(from_chips.at[c], chip_recv.at[c])
        own = parts[c, 0, pl.ds(0, seqs)] + from_pair[c, pl.ds(0, seqs)]
        for dc in range(1, chips):
            own = own + from_chips[c, dc - 1]
        for i in range(chunk // head):
            block = own[:, i * head : (i + 1) * head]
            index = c * (chunk // head) + i
            if index < q_heads:
                queries[:, index, :] = rotate(block)
            elif index < q_heads + kv_heads:
                k = index - q_heads
                turned = rotate(block)
                for g in range(group):
                    new_keys[:, k * group + g, :] = turned
            else:
                k = index - q_heads - kv_heads
                rounded = block.astype(BF16).astype(F32)
                for g in range(group):
                    new_values[:, k * group + g, :] = rounded

    column = lax.broadcasted_iota(jnp.int32, (2 * q_heads, span), 1)
    row = lax.broadcasted_iota(jnp.int32, (2 * q_heads, span), 0)
    place = jnp.where(
        column % kv_heads == row % q_heads // group,
        column // kv_heads + row // q_heads * (span // kv_heads),
        pages * page_rows,
    )
    score_scale = head ** (-0.5)
    no_query = jnp.zeros((q_heads, head), BF16)
    loads[4].wait()

    def one_sequence(s):
        query = queries[s]
        narrow = query.astype(BF16)
        paired = jnp.concatenate(
            [
                jnp.concatenate([narrow, no_query], axis=1),
                jnp.concatenate([no_query, narrow], axis=1),
            ],
            axis=0,
        )
        scores = jnp.dot(paired, key_columns[s], preferred_element_type=F32) * score_scale
        new_score = jnp.sum(query * new_keys[s], axis=1, keepdims=True) * score_scale
        masked = jnp.where(place < lengths_ref[s], scores, -jnp.inf)
        highest = jnp.max(masked, axis=1, keepdims=True)
        peak = jnp.maximum(jnp.maximum(highest[:q_heads], highest[q_heads:]), new_score)
        soft = jnp.exp(masked - jnp.concatenate([peak, peak], axis=0))
        new_weight = jnp.exp(new_score - peak)
        sums = jnp.sum(soft, axis=1, keepdims=True)
        denominator = sums[:q_heads] + sums[q_heads:] + new_weight
        result = jnp.dot(
            soft.astype(BF16), side_by_side(values, s), preferred_element_type=F32
        )
        result = result[:q_heads, :head] + result[q_heads:, head:]
        result = result + new_weight.astype(BF16).astype(F32) * new_values[s]
        mixed[s] = result / denominator

    for s in range(seqs):
        one_sequence(s)

    for h in range(q_heads):
        out_ref[:, h * head : (h + 1) * head] = mixed[:, h, :].astype(BF16)

    wait_bytes(sums_all.at[pl.ds(1, tp - 1)], sum_recv)
    grand = sums_all[0]
    for k in range(1, tp):
        grand = grand + sums_all[k]
    residual = grand / math.sqrt(total * tp)
    over = jnp.maximum(jnp.abs(residual) - TOL_STEP * counts_ref[...].astype(F32), 0.0)
    excess_ref[...] = jnp.sum(over, axis=1, keepdims=True) / math.sqrt(seqs * dp)

    wait_bytes(spread.at[pl.ds(1, dp - 1)], a2a_send)
    wait_bytes(from_pair, pair_send)
    wait_bytes(from_chips, chip_send)
    wait_bytes(sums_all.at[pl.ds(1, tp - 1)], sum_send)
    wait_bytes(excess_all.at[pl.ds(1, dp - 1)], exc_send)


def body(
    dp,
    tp,
    tokens,
    norm_gain,
    w_query,
    w_key,
    w_value,
    check_column,
    key_cache,
    value_cache,
    page_table,
    lengths,
    tol_counts,
):
    seqs, width = tokens.shape
    head = key_cache.shape[-1]
    q_width, kv_width = w_query.shape[1], w_key.shape[1]
    total = q_width + 2 * kv_width
    q_heads = q_width // head
    depth = width // dp
    chips = dp // 2
    chunks = 5 if total % (5 * head) == 0 else 1
    chunk = total // chunks
    flat_keys = key_cache.reshape(key_cache.shape[0], -1, head)
    flat_values = value_cache.reshape(value_cache.shape[0], -1, head)

    vmem = pl.BlockSpec(memory_space=pltpu.VMEM)
    hbm = pl.BlockSpec(memory_space=pltpu.HBM)
    dma = pltpu.SemaphoreType.DMA
    attention, excess = pl.pallas_call(
        functools.partial(step_kernel, dp, tp),
        out_shape=(
            pltpu.VMEM((seqs, q_width), BF16),
            pltpu.VMEM((1, 1), F32),
        ),
        in_specs=[hbm] * 11,
        out_specs=(vmem, vmem),
        scratch_shapes=[
            pltpu.SMEM(page_table.shape, jnp.int32),
            pltpu.SMEM(lengths.shape, jnp.int32),
            pltpu.VMEM((1, tol_counts.shape[0]), jnp.int32),
            pltpu.VMEM(tokens.shape, BF16),
            pltpu.VMEM((width // LANES, LANES), BF16),
            pltpu.VMEM((width // LANES, LANES), BF16),
            pltpu.VMEM((depth, total), BF16),
            pltpu.VMEM(flat_keys.shape, BF16),
            pltpu.VMEM(flat_values.shape, BF16),
            pltpu.VMEM((seqs, 2 * head, (page_table.shape[1] + 1) // 2 * flat_keys.shape[1]), BF16),
            pltpu.VMEM((dp, seqs, depth), BF16),
            pltpu.VMEM((dp, seqs, depth), BF16),
            pltpu.VMEM((chunks, 2, chips * seqs, chunk), F32),
            pltpu.VMEM((chunks, chips * seqs, chunk), F32),
            pltpu.VMEM((chunks, chips - 1, seqs, chunk), F32),
            pltpu.VMEM((seqs, q_heads, head), F32),
            pltpu.VMEM((seqs, q_heads, head), F32),
            pltpu.VMEM((seqs, q_heads, head), F32),
            pltpu.VMEM((seqs, q_heads, head), F32),
            pltpu.VMEM((tp, 1, dp * seqs), F32),
            pltpu.VMEM((1, dp * seqs), F32),
            pltpu.VMEM((dp, seqs, LANES), F32),
            pltpu.VMEM((dp, 1, dp * seqs), F32),
            pltpu.VMEM((1, dp * seqs), F32),
            dma((6,)),
            dma((3,)),
            dma(()),
            dma(()),
            dma(()),
            dma((chunks,)),
            dma(()),
            dma((chunks,)),
            dma(()),
            dma(()),
            dma(()),
            dma(()),
        ],
        compiler_params=pltpu.CompilerParams(
            collective_id=0, has_side_effects=True, vmem_limit_bytes=60 * 1024 * 1024
        ),
    )(
        page_table,
        lengths,
        tol_counts.reshape(1, -1),
        tokens,
        norm_gain.reshape(-1, LANES),
        check_column.reshape(-1, LANES),
        w_query,
        w_key,
        w_value,
        flat_keys,
        flat_values,
    )
    return attention, excess[0, 0]


def solution(mesh):
    return jax.shard_map(
        functools.partial(body, mesh.shape["dp"], mesh.shape["tensor"]),
        mesh=mesh,
        in_specs=(
            P("dp", None),
            P(),
            P("dp", "tensor"),
            P("dp", "tensor"),
            P("dp", "tensor"),
            P(),
            P("dp", None, "tensor", None),
            P("dp", None, "tensor", None),
            P("dp", None),
            P("dp"),
            P(),
        ),
        out_specs=(P("dp", "tensor"), P()),
        check_vma=False,
    )
```

```python
import functools
import math

import jax
import jax.numpy as jnp
from jax import lax
from jax.experimental import pallas as pl
from jax.experimental.pallas import tpu as pltpu
from jax.sharding import PartitionSpec as P

EPSILON = 1e-06
ROPE_BASE = 1000000.0
TOL_STEP = 0.25
MESH = pl.DeviceIdType.MESH
F32 = jnp.float32
BF16 = jnp.bfloat16
UNROLL = 4
LANES = 128
LEVELS = 32000.0
TINY = 1e-30
SPLIT = 3


def step_kernel(
    dp,
    tp,
    table_hbm,
    lengths_hbm,
    counts_hbm,
    tokens_hbm,
    gain_hbm,
    check_hbm,
    wq_hbm,
    wk_hbm,
    wv_hbm,
    keys_hbm,
    values_hbm,
    out_ref,
    excess_ref,
    table_ref,
    lengths_ref,
    counts_ref,
    tokens_ref,
    gain_ref,
    check_ref,
    weights,
    keys,
    values,
    key_columns,
    weight_sums,
    outgoing,
    spread,
    parts,
    from_pair,
    outbound,
    from_chips,
    steps_out,
    steps_in,
    queries,
    new_keys,
    new_values,
    mixed,
    sums_all,
    sums_own,
    shares,
    excess_all,
    excess_own,
    small_sems,
    load_sems,
    a2a_send,
    a2a_recv,
    pair_send,
    pair_recv,
    chip_send,
    chip_recv,
    step_send,
    step_recv,
    sum_send,
    sum_recv,
    exc_send,
    exc_recv,
):
    chips = dp // 2
    spread_lanes = steps_out.shape[2]
    me = lax.axis_index("dp")
    zed = lax.axis_index("tensor")
    chip, core = me // 2, me % 2
    seqs, width = tokens_ref.shape
    depth = width // dp
    q_width, kv_width = wq_hbm.shape[1], wk_hbm.shape[1]
    total = q_width + 2 * kv_width
    chunks, _, _, chunk = parts.shape
    head = keys_hbm.shape[2]
    q_heads, kv_heads = q_width // head, kv_width // head
    group = q_heads // kv_heads
    pages = table_ref.shape[1]
    page_rows = keys_hbm.shape[1]

    def wait_bytes(ref, sem):
        pltpu.make_async_copy(ref, ref, sem).wait()

    def partner(dc):
        other, bit = chip, 1
        while bit <= dc:
            if dc // bit % 2:
                other = other + bit - 2 * bit * (chip // bit % 2)
            bit *= 2
        return other

    barrier = pltpu.get_barrier_semaphore()
    for k in range(1, dp):
        pl.semaphore_signal(
            barrier, inc=1, device_id=((me + k) % dp, zed), device_id_type=MESH
        )

    small_loads = [
        pltpu.make_async_copy(source, target, small_sems.at[i])
        for i, (source, target) in enumerate(
            [
                (tokens_hbm, tokens_ref),
                (gain_hbm, gain_ref),
                (lengths_hbm, lengths_ref),
                (table_hbm, table_ref),
                (counts_hbm, counts_ref),
                (check_hbm, check_ref),
            ]
        )
    ]
    for load in small_loads:
        load.start()
    loads = [
        pltpu.make_async_copy(keys_hbm, keys, load_sems.at[1]),
        pltpu.make_async_copy(wq_hbm, weights.at[:, pl.ds(0, q_width)], load_sems.at[0]),
        pltpu.make_async_copy(wk_hbm, weights.at[:, pl.ds(q_width, kv_width)], load_sems.at[0]),
        pltpu.make_async_copy(
            wv_hbm, weights.at[:, pl.ds(q_width + kv_width, kv_width)], load_sems.at[0]
        ),
        pltpu.make_async_copy(values_hbm, values, load_sems.at[2]),
    ]

    loads[0].start()
    for load in small_loads[:2]:
        load.wait()
    for load in loads[1:4]:
        load.start()
    square = jnp.zeros((seqs, LANES), F32)
    for j in range(width // LANES):
        part = tokens_ref[:, j * LANES : (j + 1) * LANES].astype(F32)
        square = square + part * part
    scale = lax.rsqrt(jnp.sum(square, axis=1, keepdims=True) / width + EPSILON)
    gains = gain_ref[...].astype(F32)
    for j in range(width // LANES):
        part = tokens_ref[:, j * LANES : (j + 1) * LANES].astype(F32)
        at = j * LANES % depth
        outgoing[j * LANES // depth, :, at : at + LANES] = (
            part * scale * gains[j : j + 1]
        ).astype(BF16)
    spread[0] = outgoing[me]

    pl.semaphore_wait(barrier, dp - 1 + (zed + tp - 1) // tp)

    def greet_plane(k):
        @pl.when((zed + k >= 0) & (zed + k < tp))
        def _():
            pl.semaphore_signal(barrier, inc=1, device_id=(me, zed + k), device_id_type=MESH)


    for dc in range(chips - 1, -1, -1):
        for q in range(2):
            if dc == 0 and q == 0:
                continue
            target = partner(dc) * 2 + (core + q) % 2
            copy = pltpu.make_async_remote_copy(
                src_ref=outgoing.at[target],
                dst_ref=spread.at[q * chips + dc],
                send_sem=a2a_send,
                recv_sem=a2a_recv,
                device_id=(target, zed),
                device_id_type=MESH,
            )
            copy.start()

    greet_plane(1)
    for k in range(1, tp):
        greet_plane(-k)

    for load in small_loads[2:5]:
        load.wait()
    seq_row = lax.broadcasted_iota(jnp.int32, (seqs, LANES), 0)
    positions = jnp.zeros((seqs, LANES), F32)
    for s in range(seqs):
        positions = jnp.where(seq_row == s, lengths_ref[s].astype(F32), positions)
    lane = lax.broadcasted_iota(jnp.int32, (seqs, head), 1)
    step = (lane % (head // 2)).astype(F32)
    angles = positions * jnp.exp(step * (-2.0 * math.log(ROPE_BASE) / head))
    cosine = jnp.cos(angles)
    sine = jnp.where(lane < head // 2, -1.0, 1.0) * jnp.sin(angles)

    near = (pages + 1) // 2
    far = pages - near
    span = near * page_rows
    no_page = jnp.zeros((page_rows, head), BF16)

    def side_by_side(pool, s):
        left = [pool[table_ref[s, p]] for p in range(near)]
        right = [pool[table_ref[s, p]] for p in range(near, pages)] + [no_page] * (near - far)
        return jnp.concatenate(
            [jnp.concatenate(left, axis=0), jnp.concatenate(right, axis=0)], axis=1
        )

    def turn_keys(s, carry):
        key_columns[s] = jnp.transpose(side_by_side(keys, s))
        return carry

    loads[0].wait()
    loads[4].start()
    lax.fori_loop(0, seqs, turn_keys, 0, unroll=UNROLL)

    small_loads[5].wait()
    checks = check_ref[...].astype(F32)
    checked = jnp.zeros((seqs, LANES), F32)
    for j in range(width // LANES):
        at = j * LANES % depth
        part = outgoing[j * LANES // depth, :, at : at + LANES].astype(F32)
        checked = checked + part * checks[j : j + 1]

    wait_bytes(weights, load_sems.at[0])

    def sum_weights(i, carry):
        rows = pl.ds(i * 2 * LANES, 2 * LANES)
        part = weights[rows, pl.ds(0, LANES)].astype(F32)
        for j in range(1, total // LANES):
            part = part + weights[rows, pl.ds(j * LANES, LANES)].astype(F32)
        for term in range(SPLIT):
            rounded = part.astype(BF16)
            weight_sums[rows, pl.ds(term * LANES, LANES)] = rounded
            part = part - rounded.astype(F32)
        return carry

    lax.fori_loop(0, depth // (2 * LANES), sum_weights, 0)

    wait_bytes(spread.at[pl.ds(1, dp - 1)], a2a_recv)

    pair_copies = []
    half = chips * seqs

    def project(c):
        product = jnp.dot(
            spread[...].reshape(dp * seqs, depth),
            weights[:, pl.ds(c * chunk, chunk)],
            preferred_element_type=F32,
        )
        parts[c, 1] = product[half:]
        copy = pltpu.make_async_remote_copy(
            src_ref=parts.at[c, 1],
            dst_ref=from_pair.at[c],
            send_sem=pair_send,
            recv_sem=pair_recv.at[c],
            device_id=(chip * 2 + (core + 1) % 2, zed),
            device_id_type=MESH,
        )
        copy.start()
        pair_copies.append(copy)
        parts[c, 0] = product[:half]

    spots = lax.broadcasted_iota(jnp.int32, (half - seqs, spread_lanes), 1)
    spot_rows = lax.broadcasted_iota(jnp.int32, (half - seqs, spread_lanes), 0)

    def pass_on(c):
        pair_copies[c].wait_recv()
        summed = parts[c, 0, pl.ds(seqs, half - seqs)] + from_pair[c, pl.ds(seqs, half - seqs)]
        largest = jnp.max(jnp.abs(summed), axis=1, keepdims=True)
        step = (jnp.maximum(largest, TINY) * (1.0 / LEVELS)).astype(BF16).astype(F32)
        coded = jnp.round(summed * (1.0 / step)).astype(jnp.int32).astype(jnp.int16)
        for dc in range(1, chips):
            rows = slice((dc - 1) * seqs, dc * seqs)
            outbound[c, dc - 1] = coded[rows]
        steps_out[c] = jnp.sum(jnp.where(spots == spot_rows, step, 0.0), axis=0, keepdims=True)
        for dc in range(chips - 1, 0, -1):
            send_on(steps_out.at[c], steps_in.at[c, dc - 1], step_send, step_recv.at[c], dc)
            send_on(
                outbound.at[c, dc - 1], from_chips.at[c, dc - 1], chip_send, chip_recv.at[c], dc
            )

    def send_on(source, target, send_sem, recv_sem, dc):
        pltpu.make_async_remote_copy(
            src_ref=source,
            dst_ref=target,
            send_sem=send_sem,
            recv_sem=recv_sem,
            device_id=(partner(dc) * 2 + core, zed),
            device_id_type=MESH,
        ).start()

    def exchange(own, everyone, place, targets, send_sem, recv_sem):
        everyone[place] = own[...]
        for target in targets:
            pltpu.make_async_remote_copy(
                src_ref=own,
                dst_ref=everyone.at[place],
                send_sem=send_sem,
                recv_sem=recv_sem,
                device_id=target,
                device_id_type=MESH,
            ).start()

    def send_sums():
        sum_terms = jnp.dot(
            spread[...].reshape(dp * seqs, depth), weight_sums[...], preferred_element_type=F32
        )
        row_sum = sum(sum_terms[:, i * LANES : (i + 1) * LANES] for i in range(SPLIT))
        for q in range(2):
            for dc in range(chips):
                owner = partner(dc) * 2 + (core + q) % 2
                at = (q * chips + dc) * seqs
                share = row_sum[at : at + seqs]
                if q == 0 and dc == 0:
                    share = share - jnp.where(zed == 0, checked, 0.0)
                shares[owner] = share
        turned_sums = jnp.transpose(shares[...].reshape(dp * seqs, LANES))
        excess_own[...] = jnp.sum(turned_sums, axis=0, keepdims=True)
        exchange(
            excess_own, excess_all, me, [((me + k) % dp, zed) for k in range(1, dp)], exc_send, exc_recv
        )

    for c in range(chunks + 3):
        if c < chunks:
            project(c)
        if c == 1:
            send_sums()
        if c >= 2 and c - 2 < chunks:
            pass_on(c - 2)
    wait_bytes(excess_all.at[pl.ds(1, dp - 1)], exc_recv)
    group_sum = excess_all[0]
    for k in range(1, dp):
        group_sum = group_sum + excess_all[k]
    sums_own[...] = group_sum

    @pl.when(zed < tp - 1)
    def _():
        pl.semaphore_wait(barrier, tp - 1 - zed)

    exchange(
        sums_own, sums_all, zed, [(me, (zed + k) % tp) for k in range(1, tp)], sum_send, sum_recv
    )


    def rotate(vector):
        return (
            (vector * cosine + pltpu.roll(vector, head // 2, 1) * sine)
            .astype(BF16)
            .astype(F32)
        )

    for c in range(chunks):
        wait_bytes(steps_in.at[c], step_recv.at[c])
        wait_bytes(from_chips.at[c], chip_recv.at[c])
        own = parts[c, 0, pl.ds(0, seqs)] + from_pair[c, pl.ds(0, seqs)]
        for dc in range(1, chips):
            spot = spot_rows[:seqs] + (dc - 1) * seqs
            step = jnp.sum(
                jnp.where(spots[:seqs] == spot, steps_in[c, dc - 1], 0.0), axis=1, keepdims=True
            )
            own = own + from_chips[c, dc - 1].astype(jnp.int32).astype(F32) * step
        for i in range(chunk // head):
            block = own[:, i * head : (i + 1) * head]
            index = c * (chunk // head) + i
            if index < q_heads:
                queries[:, index, :] = rotate(block)
            elif index < q_heads + kv_heads:
                k = index - q_heads
                turned = rotate(block)
                for g in range(group):
                    new_keys[:, k * group + g, :] = turned
            else:
                k = index - q_heads - kv_heads
                rounded = block.astype(BF16).astype(F32)
                for g in range(group):
                    new_values[:, k * group + g, :] = rounded

    column = lax.broadcasted_iota(jnp.int32, (2 * q_heads, span), 1)
    row = lax.broadcasted_iota(jnp.int32, (2 * q_heads, span), 0)
    place = jnp.where(
        column % kv_heads == row % q_heads // group,
        column // kv_heads + row // q_heads * (span // kv_heads),
        pages * page_rows,
    )
    score_scale = head ** (-0.5)
    no_query = jnp.zeros((q_heads, head), BF16)
    loads[4].wait()

    def one_sequence(s):
        query = queries[s]
        narrow = query.astype(BF16)
        paired = jnp.concatenate(
            [
                jnp.concatenate([narrow, no_query], axis=1),
                jnp.concatenate([no_query, narrow], axis=1),
            ],
            axis=0,
        )
        scores = jnp.dot(paired, key_columns[s], preferred_element_type=F32) * score_scale
        new_score = jnp.sum(query * new_keys[s], axis=1, keepdims=True) * score_scale
        masked = jnp.where(place < lengths_ref[s], scores, -jnp.inf)
        highest = jnp.max(masked, axis=1, keepdims=True)
        peak = jnp.maximum(jnp.maximum(highest[:q_heads], highest[q_heads:]), new_score)
        soft = jnp.exp(masked - jnp.concatenate([peak, peak], axis=0))
        new_weight = jnp.exp(new_score - peak)
        sums = jnp.sum(soft, axis=1, keepdims=True)
        denominator = sums[:q_heads] + sums[q_heads:] + new_weight
        result = jnp.dot(
            soft.astype(BF16), side_by_side(values, s), preferred_element_type=F32
        )
        result = result[:q_heads, :head] + result[q_heads:, head:]
        result = result + new_weight.astype(BF16).astype(F32) * new_values[s]
        mixed[s] = result / denominator

    for s in range(seqs):
        one_sequence(s)

    for h in range(q_heads):
        out_ref[:, h * head : (h + 1) * head] = mixed[:, h, :].astype(BF16)

    wait_bytes(sums_all.at[pl.ds(1, tp - 1)], sum_recv)
    grand = sums_all[0]
    for k in range(1, tp):
        grand = grand + sums_all[k]
    residual = grand / math.sqrt(total * tp)
    over = jnp.maximum(jnp.abs(residual) - TOL_STEP * counts_ref[...].astype(F32), 0.0)
    excess_ref[...] = jnp.sum(over, axis=1, keepdims=True) / math.sqrt(seqs * dp)

    wait_bytes(spread.at[pl.ds(1, dp - 1)], a2a_send)
    wait_bytes(from_pair, pair_send)
    wait_bytes(from_chips, chip_send)
    wait_bytes(steps_in, step_send)
    wait_bytes(sums_all.at[pl.ds(1, tp - 1)], sum_send)
    wait_bytes(excess_all.at[pl.ds(1, dp - 1)], exc_send)


def body(
    dp,
    tp,
    tokens,
    norm_gain,
    w_query,
    w_key,
    w_value,
    check_column,
    key_cache,
    value_cache,
    page_table,
    lengths,
    tol_counts,
):
    seqs, width = tokens.shape
    head = key_cache.shape[-1]
    q_width, kv_width = w_query.shape[1], w_key.shape[1]
    total = q_width + 2 * kv_width
    q_heads = q_width // head
    depth = width // dp
    chips = dp // 2
    chunks = 5 if total % (5 * head) == 0 else 1
    chunk = total // chunks
    spread_lanes = -(-(chips - 1) * seqs // LANES) * LANES
    flat_keys = key_cache.reshape(key_cache.shape[0], -1, head)
    flat_values = value_cache.reshape(value_cache.shape[0], -1, head)

    vmem = pl.BlockSpec(memory_space=pltpu.VMEM)
    hbm = pl.BlockSpec(memory_space=pltpu.HBM)
    dma = pltpu.SemaphoreType.DMA
    attention, excess = pl.pallas_call(
        functools.partial(step_kernel, dp, tp),
        out_shape=(
            pltpu.VMEM((seqs, q_width), BF16),
            pltpu.VMEM((1, 1), F32),
        ),
        in_specs=[hbm] * 11,
        out_specs=(vmem, vmem),
        scratch_shapes=[
            pltpu.SMEM(page_table.shape, jnp.int32),
            pltpu.SMEM(lengths.shape, jnp.int32),
            pltpu.VMEM((1, tol_counts.shape[0]), jnp.int32),
            pltpu.VMEM(tokens.shape, BF16),
            pltpu.VMEM((width // LANES, LANES), BF16),
            pltpu.VMEM((width // LANES, LANES), BF16),
            pltpu.VMEM((depth, total), BF16),
            pltpu.VMEM(flat_keys.shape, BF16),
            pltpu.VMEM(flat_values.shape, BF16),
            pltpu.VMEM((seqs, 2 * head, (page_table.shape[1] + 1) // 2 * flat_keys.shape[1]), BF16),
            pltpu.VMEM((depth, SPLIT * LANES), BF16),
            pltpu.VMEM((dp, seqs, depth), BF16),
            pltpu.VMEM((dp, seqs, depth), BF16),
            pltpu.VMEM((chunks, 2, chips * seqs, chunk), F32),
            pltpu.VMEM((chunks, chips * seqs, chunk), F32),
            pltpu.VMEM((chunks, chips - 1, seqs, chunk), jnp.int16),
            pltpu.VMEM((chunks, chips - 1, seqs, chunk), jnp.int16),
            pltpu.VMEM((chunks, 1, spread_lanes), F32),
            pltpu.VMEM((chunks, chips - 1, 1, spread_lanes), F32),
            pltpu.VMEM((seqs, q_heads, head), F32),
            pltpu.VMEM((seqs, q_heads, head), F32),
            pltpu.VMEM((seqs, q_heads, head), F32),
            pltpu.VMEM((seqs, q_heads, head), F32),
            pltpu.VMEM((tp, 1, dp * seqs), F32),
            pltpu.VMEM((1, dp * seqs), F32),
            pltpu.VMEM((dp, seqs, LANES), F32),
            pltpu.VMEM((dp, 1, dp * seqs), F32),
            pltpu.VMEM((1, dp * seqs), F32),
            dma((6,)),
            dma((3,)),
            dma(()),
            dma(()),
            dma(()),
            dma((chunks,)),
            dma(()),
            dma((chunks,)),
            dma(()),
            dma((chunks,)),
            dma(()),
            dma(()),
            dma(()),
            dma(()),
        ],
        compiler_params=pltpu.CompilerParams(
            collective_id=0, has_side_effects=True, vmem_limit_bytes=60 * 1024 * 1024
        ),
    )(
        page_table,
        lengths,
        tol_counts.reshape(1, -1),
        tokens,
        norm_gain.reshape(-1, LANES),
        check_column.reshape(-1, LANES),
        w_query,
        w_key,
        w_value,
        flat_keys,
        flat_values,
    )
    return attention, excess[0, 0]


def solution(mesh):
    return jax.shard_map(
        functools.partial(body, mesh.shape["dp"], mesh.shape["tensor"]),
        mesh=mesh,
        in_specs=(
            P("dp", None),
            P(),
            P("dp", "tensor"),
            P("dp", "tensor"),
            P("dp", "tensor"),
            P(),
            P("dp", None, "tensor", None),
            P("dp", None, "tensor", None),
            P("dp", None),
            P("dp"),
            P(),
        ),
        out_specs=(P("dp", "tensor"), P()),
        check_vma=False,
    )
```

```python
import functools
import math

import jax
import jax.numpy as jnp
from jax import lax
from jax.experimental import pallas as pl
from jax.experimental.pallas import tpu as pltpu
from jax.sharding import PartitionSpec as P

EPSILON = 1e-06
ROPE_BASE = 1000000.0
TOL_STEP = 0.25
MESH = pl.DeviceIdType.MESH
F32 = jnp.float32
BF16 = jnp.bfloat16
UNROLL = 4
LANES = 128
LEVELS = 32000.0
TINY = 1e-30
SPLIT = 3


def step_kernel(
    dp,
    tp,
    table_hbm,
    lengths_hbm,
    counts_hbm,
    tokens_hbm,
    gain_hbm,
    check_hbm,
    wq_hbm,
    wk_hbm,
    wv_hbm,
    keys_hbm,
    values_hbm,
    out_ref,
    excess_ref,
    table_ref,
    lengths_ref,
    counts_ref,
    tokens_ref,
    gain_ref,
    check_ref,
    weights,
    keys,
    values,
    key_columns,
    weight_sums,
    check_row,
    outgoing,
    spread,
    parts,
    from_pair,
    outbound,
    from_chips,
    steps_out,
    steps_in,
    queries,
    new_keys,
    new_values,
    mixed,
    sums_all,
    sums_own,
    shares,
    excess_all,
    excess_own,
    small_sems,
    load_sems,
    a2a_send,
    a2a_recv,
    pair_send,
    pair_recv,
    chip_send,
    chip_recv,
    step_send,
    step_recv,
    sum_send,
    sum_recv,
    exc_send,
    exc_recv,
):
    chips = dp // 2
    spread_lanes = steps_out.shape[2]
    me = lax.axis_index("dp")
    zed = lax.axis_index("tensor")
    chip, core = me // 2, me % 2
    seqs, width = tokens_ref.shape
    depth = width // dp
    q_width, kv_width = wq_hbm.shape[1], wk_hbm.shape[1]
    total = q_width + 2 * kv_width
    chunks, _, _, chunk = parts.shape
    head = keys_hbm.shape[2]
    q_heads, kv_heads = q_width // head, kv_width // head
    group = q_heads // kv_heads
    pages = table_ref.shape[1]
    page_rows = keys_hbm.shape[1]

    def wait_bytes(ref, sem):
        pltpu.make_async_copy(ref, ref, sem).wait()

    def partner(dc):
        other, bit = chip, 1
        while bit <= dc:
            if dc // bit % 2:
                other = other + bit - 2 * bit * (chip // bit % 2)
            bit *= 2
        return other

    def slot(q, dc):
        return (1 - q if dc else q) * chips + dc

    barrier = pltpu.get_barrier_semaphore()
    for k in range(1, dp):
        pl.semaphore_signal(
            barrier, inc=1, device_id=((me + k) % dp, zed), device_id_type=MESH
        )

    small_loads = [
        pltpu.make_async_copy(source, target, small_sems.at[i])
        for i, (source, target) in enumerate(
            [
                (tokens_hbm, tokens_ref),
                (gain_hbm, gain_ref),
                (lengths_hbm, lengths_ref),
                (table_hbm, table_ref),
                (counts_hbm, counts_ref),
                (check_hbm, check_ref),
            ]
        )
    ]
    for load in small_loads:
        load.start()
    loads = [
        pltpu.make_async_copy(keys_hbm, keys, load_sems.at[1]),
        pltpu.make_async_copy(wq_hbm, weights.at[:, pl.ds(0, q_width)], load_sems.at[0]),
        pltpu.make_async_copy(wk_hbm, weights.at[:, pl.ds(q_width, kv_width)], load_sems.at[0]),
        pltpu.make_async_copy(
            wv_hbm, weights.at[:, pl.ds(q_width + kv_width, kv_width)], load_sems.at[0]
        ),
        pltpu.make_async_copy(values_hbm, values, load_sems.at[2]),
    ]

    loads[0].start()
    for load in small_loads[:2]:
        load.wait()
    for load in loads[1:4]:
        load.start()
    square = jnp.zeros((seqs, LANES), F32)
    for j in range(width // LANES):
        part = tokens_ref[:, j * LANES : (j + 1) * LANES].astype(F32)
        square = square + part * part
    scale = lax.rsqrt(jnp.sum(square, axis=1, keepdims=True) / width + EPSILON)
    gains = gain_ref[...].astype(F32)
    for j in range(width // LANES):
        part = tokens_ref[:, j * LANES : (j + 1) * LANES].astype(F32)
        at = j * LANES % depth
        outgoing[j * LANES // depth, :, at : at + LANES] = (
            part * scale * gains[j : j + 1]
        ).astype(BF16)
    spread[0] = outgoing[me]

    pl.semaphore_wait(barrier, dp - 1 + (zed + tp - 1) // tp)

    def greet_plane(k):
        @pl.when((zed + k >= 0) & (zed + k < tp))
        def _():
            pl.semaphore_signal(barrier, inc=1, device_id=(me, zed + k), device_id_type=MESH)


    for dc in range(chips - 1, -1, -1):
        for there in range(2) if dc else [1 - core]:
            q = (there + core) % 2
            target = partner(dc) * 2 + there
            copy = pltpu.make_async_remote_copy(
                src_ref=outgoing.at[target],
                dst_ref=spread.at[slot(q, dc)],
                send_sem=a2a_send,
                recv_sem=a2a_recv,
                device_id=(target, zed),
                device_id_type=MESH,
            )
            copy.start()

    greet_plane(1)
    for k in range(1, tp):
        greet_plane(-k)

    for load in small_loads[2:5]:
        load.wait()
    seq_row = lax.broadcasted_iota(jnp.int32, (seqs, LANES), 0)
    positions = jnp.zeros((seqs, LANES), F32)
    for s in range(seqs):
        positions = jnp.where(seq_row == s, lengths_ref[s].astype(F32), positions)
    lane = lax.broadcasted_iota(jnp.int32, (seqs, head), 1)
    step = (lane % (head // 2)).astype(F32)
    angles = positions * jnp.exp(step * (-2.0 * math.log(ROPE_BASE) / head))
    cosine = jnp.cos(angles)
    sine = jnp.where(lane < head // 2, -1.0, 1.0) * jnp.sin(angles)

    near = (pages + 1) // 2
    far = pages - near
    span = near * page_rows
    no_page = jnp.zeros((page_rows, head), BF16)

    def side_by_side(pool, s):
        left = [pool[table_ref[s, p]] for p in range(near)]
        right = [pool[table_ref[s, p]] for p in range(near, pages)] + [no_page] * (near - far)
        return jnp.concatenate(
            [jnp.concatenate(left, axis=0), jnp.concatenate(right, axis=0)], axis=1
        )

    def turn_keys(s, carry):
        key_columns[s] = jnp.transpose(side_by_side(keys, s))
        return carry

    loads[0].wait()
    loads[4].start()
    lax.fori_loop(0, seqs, turn_keys, 0, unroll=UNROLL)

    small_loads[5].wait()
    checks = check_ref[...].astype(F32)
    checked = jnp.zeros((seqs, LANES), F32)
    for j in range(width // LANES):
        at = j * LANES % depth
        part = outgoing[j * LANES // depth, :, at : at + LANES].astype(F32)
        checked = checked + part * checks[j : j + 1]
    shares[...] = jnp.zeros(shares.shape, F32)
    shares[me] = jnp.where(zed == 0, checked, 0.0)
    turned_checks = jnp.transpose(shares[...].reshape(dp * seqs, LANES))
    check_row[...] = jnp.sum(turned_checks, axis=0, keepdims=True)

    wait_bytes(weights, load_sems.at[0])

    totals = lax.dot_general(
        jnp.ones((seqs, total), BF16),
        weights[...],
        (((1,), (1,)), ((), ())),
        preferred_element_type=F32,
    )
    term = lax.broadcasted_iota(jnp.int32, (seqs, depth), 0)
    split = jnp.zeros((seqs, depth), F32)
    for i in range(SPLIT):
        rounded = totals.astype(BF16).astype(F32)
        split = jnp.where(term == i, rounded, split)
        totals = totals - rounded
    weight_sums[...] = split.astype(BF16)

    wait_bytes(spread.at[pl.ds(1, dp - 1)], a2a_recv)

    pair_copies = []
    batch = seqs // 2
    half = chips * seqs

    def project(c):
        product = jnp.dot(
            spread[...].reshape(dp * seqs, depth),
            weights[:, pl.ds(c * chunk, chunk)],
            preferred_element_type=F32,
        )
        parts[c, 1] = product[half:]
        copy = pltpu.make_async_remote_copy(
            src_ref=parts.at[c, 1],
            dst_ref=from_pair.at[c],
            send_sem=pair_send,
            recv_sem=pair_recv.at[c],
            device_id=(chip * 2 + (core + 1) % 2, zed),
            device_id_type=MESH,
        )
        copy.start()
        pair_copies.append(copy)
        parts[c, 0] = product[:half]

    spots = lax.broadcasted_iota(jnp.int32, (half - seqs, spread_lanes), 1)
    spot_rows = lax.broadcasted_iota(jnp.int32, (half - seqs, spread_lanes), 0)

    def pass_on(c):
        pair_copies[c].wait_recv()
        summed = parts[c, 0, pl.ds(seqs, half - seqs)] + from_pair[c, pl.ds(seqs, half - seqs)]
        largest = jnp.max(jnp.abs(summed), axis=1, keepdims=True)
        step = (jnp.maximum(largest, TINY) * (1.0 / LEVELS)).astype(BF16).astype(F32)
        coded = jnp.round(summed * (1.0 / step)).astype(jnp.int32)
        for dc in range(1, chips):
            for h in range(2):
                at = (dc - 1) * seqs + h * batch
                stacked = jnp.concatenate(
                    [coded[at : at + batch, : chunk // 2], coded[at : at + batch, chunk // 2 :]],
                    axis=0,
                )
                outbound[h, c, dc - 1] = stacked.astype(jnp.int16)
        steps_out[c] = jnp.sum(jnp.where(spots == spot_rows, step, 0.0), axis=0, keepdims=True)
        for dc in range(chips - 1, 0, -1):
            send_on(steps_out.at[c], steps_in.at[c, dc - 1], step_send, step_recv.at[c], dc)
        send_batch(0, c)

    def send_batch(h, c):
        for dc in range(chips - 1, 0, -1):
            send_on(
                outbound.at[h, c, dc - 1],
                from_chips.at[h, c, dc - 1],
                chip_send,
                chip_recv.at[c if h == 0 else chunks],
                dc,
            )

    def send_on(source, target, send_sem, recv_sem, dc):
        pltpu.make_async_remote_copy(
            src_ref=source,
            dst_ref=target,
            send_sem=send_sem,
            recv_sem=recv_sem,
            device_id=(partner(dc) * 2 + (core + 1) % 2, zed),
            device_id_type=MESH,
        ).start()

    def exchange(own, everyone, place, targets, send_sem, recv_sem):
        everyone[place] = own[...]
        for target in targets:
            pltpu.make_async_remote_copy(
                src_ref=own,
                dst_ref=everyone.at[place],
                send_sem=send_sem,
                recv_sem=recv_sem,
                device_id=target,
                device_id_type=MESH,
            ).start()

    def send_sums():
        blocks = []
        for owner in range(dp):
            there = owner // 2
            relative, bit = 0, 1
            while bit < chips:
                mine, other = chip // bit % 2, there // bit % 2
                relative = relative + bit * ((mine + other) % 2)
                bit *= 2
            kept = (core + owner + (relative + chips - 1) // chips) % 2
            blocks.append(spread[kept * chips + relative])
        terms = lax.dot_general(
            weight_sums[...],
            jnp.concatenate(blocks, axis=0),
            (((1,), (1,)), ((), ())),
            preferred_element_type=F32,
        )
        excess_own[...] = jnp.sum(terms, axis=0, keepdims=True) - check_row[...]
        exchange(
            excess_own, excess_all, me, [((me + k) % dp, zed) for k in range(1, dp)], exc_send, exc_recv
        )

    for c in range(chunks):
        project(c)
        if c == 0:
            send_sums()
        if c >= 3:
            pass_on(c - 3)
    for c in range(max(chunks - 3, 0), chunks):
        pass_on(c)
    for c in range(chunks):
        send_batch(1, c)

    def finish_group():
        wait_bytes(excess_all.at[pl.ds(1, dp - 1)], exc_recv)
        group_sum = excess_all[0]
        for k in range(1, dp):
            group_sum = group_sum + excess_all[k]
        sums_own[...] = group_sum

        @pl.when(zed < tp - 1)
        def _():
            pl.semaphore_wait(barrier, tp - 1 - zed)

        exchange(
            sums_own, sums_all, zed, [(me, (zed + k) % tp) for k in range(1, tp)], sum_send, sum_recv
        )

    def rotate(vector, rows):
        return (
            (vector * cosine[rows] + pltpu.roll(vector, head // 2, 1) * sine[rows])
            .astype(BF16)
            .astype(F32)
        )

    def settle(h, c):
        if h == 0:
            wait_bytes(steps_in.at[c], step_recv.at[c])
            wait_bytes(from_chips.at[h, c], chip_recv.at[c])
        rows = slice(h * batch, (h + 1) * batch)
        own = parts[c, 0, rows] + from_pair[c, rows]
        for dc in range(1, chips):
            spot = spot_rows[rows] + (dc - 1) * seqs
            step = jnp.sum(
                jnp.where(spots[rows] == spot, steps_in[c, dc - 1], 0.0), axis=1, keepdims=True
            )
            stacked = from_chips[h, c, dc - 1].astype(jnp.int32).astype(F32)
            own = own + jnp.concatenate([stacked[:batch], stacked[batch:]], axis=1) * step
        for i in range(chunk // head):
            block = own[:, i * head : (i + 1) * head]
            index = c * (chunk // head) + i
            if index < q_heads:
                queries[rows, index, :] = rotate(block, rows)
            elif index < q_heads + kv_heads:
                k = index - q_heads
                turned = rotate(block, rows)
                for g in range(group):
                    new_keys[rows, k * group + g, :] = turned
            else:
                k = index - q_heads - kv_heads
                rounded = block.astype(BF16).astype(F32)
                for g in range(group):
                    new_values[rows, k * group + g, :] = rounded

    column = lax.broadcasted_iota(jnp.int32, (2 * q_heads, span), 1)
    row = lax.broadcasted_iota(jnp.int32, (2 * q_heads, span), 0)
    place = jnp.where(
        column % kv_heads == row % q_heads // group,
        column // kv_heads + row // q_heads * (span // kv_heads),
        pages * page_rows,
    )
    score_scale = head ** (-0.5)
    no_query = jnp.zeros((q_heads, head), BF16)
    loads[4].wait()

    def one_sequence(s):
        query = queries[s]
        narrow = query.astype(BF16)
        paired = jnp.concatenate(
            [
                jnp.concatenate([narrow, no_query], axis=1),
                jnp.concatenate([no_query, narrow], axis=1),
            ],
            axis=0,
        )
        scores = jnp.dot(paired, key_columns[s], preferred_element_type=F32) * score_scale
        new_score = jnp.sum(query * new_keys[s], axis=1, keepdims=True) * score_scale
        masked = jnp.where(place < lengths_ref[s], scores, -jnp.inf)
        highest = jnp.max(masked, axis=1, keepdims=True)
        peak = jnp.maximum(jnp.maximum(highest[:q_heads], highest[q_heads:]), new_score)
        soft = jnp.exp(masked - jnp.concatenate([peak, peak], axis=0))
        new_weight = jnp.exp(new_score - peak)
        sums = jnp.sum(soft, axis=1, keepdims=True)
        denominator = sums[:q_heads] + sums[q_heads:] + new_weight
        result = jnp.dot(
            soft.astype(BF16), side_by_side(values, s), preferred_element_type=F32
        )
        result = result[:q_heads, :head] + result[q_heads:, head:]
        result = result + new_weight.astype(BF16).astype(F32) * new_values[s]
        mixed[s] = result / denominator

    for h in range(2):
        if h == 0:
            finish_group()
        else:
            wait_bytes(from_chips.at[1], chip_recv.at[chunks])
        for c in range(chunks):
            settle(h, c)
        for s in range(h * batch, (h + 1) * batch):
            one_sequence(s)

    for h in range(q_heads):
        out_ref[:, h * head : (h + 1) * head] = mixed[:, h, :].astype(BF16)

    wait_bytes(sums_all.at[pl.ds(1, tp - 1)], sum_recv)
    grand = sums_all[0]
    for k in range(1, tp):
        grand = grand + sums_all[k]
    residual = grand / math.sqrt(total * tp)
    over = jnp.maximum(jnp.abs(residual) - TOL_STEP * counts_ref[...].astype(F32), 0.0)
    excess_ref[...] = jnp.sum(over, axis=1, keepdims=True) / math.sqrt(seqs * dp)

    wait_bytes(spread.at[pl.ds(1, dp - 1)], a2a_send)
    wait_bytes(from_pair, pair_send)
    wait_bytes(from_chips, chip_send)
    wait_bytes(steps_in, step_send)
    wait_bytes(sums_all.at[pl.ds(1, tp - 1)], sum_send)
    wait_bytes(excess_all.at[pl.ds(1, dp - 1)], exc_send)


def body(
    dp,
    tp,
    tokens,
    norm_gain,
    w_query,
    w_key,
    w_value,
    check_column,
    key_cache,
    value_cache,
    page_table,
    lengths,
    tol_counts,
):
    seqs, width = tokens.shape
    head = key_cache.shape[-1]
    q_width, kv_width = w_query.shape[1], w_key.shape[1]
    total = q_width + 2 * kv_width
    q_heads = q_width // head
    depth = width // dp
    chips = dp // 2
    chunks = 5 if total % (5 * head) == 0 else 1
    chunk = total // chunks
    spread_lanes = -(-(chips - 1) * seqs // LANES) * LANES
    flat_keys = key_cache.reshape(key_cache.shape[0], -1, head)
    flat_values = value_cache.reshape(value_cache.shape[0], -1, head)

    vmem = pl.BlockSpec(memory_space=pltpu.VMEM)
    hbm = pl.BlockSpec(memory_space=pltpu.HBM)
    dma = pltpu.SemaphoreType.DMA
    attention, excess = pl.pallas_call(
        functools.partial(step_kernel, dp, tp),
        out_shape=(
            pltpu.VMEM((seqs, q_width), BF16),
            pltpu.VMEM((1, 1), F32),
        ),
        in_specs=[hbm] * 11,
        out_specs=(vmem, vmem),
        scratch_shapes=[
            pltpu.SMEM(page_table.shape, jnp.int32),
            pltpu.SMEM(lengths.shape, jnp.int32),
            pltpu.VMEM((1, tol_counts.shape[0]), jnp.int32),
            pltpu.VMEM(tokens.shape, BF16),
            pltpu.VMEM((width // LANES, LANES), BF16),
            pltpu.VMEM((width // LANES, LANES), BF16),
            pltpu.VMEM((depth, total), BF16),
            pltpu.VMEM(flat_keys.shape, BF16),
            pltpu.VMEM(flat_values.shape, BF16),
            pltpu.VMEM((seqs, 2 * head, (page_table.shape[1] + 1) // 2 * flat_keys.shape[1]), BF16),
            pltpu.VMEM((seqs, depth), BF16),
            pltpu.VMEM((1, dp * seqs), F32),
            pltpu.VMEM((dp, seqs, depth), BF16),
            pltpu.VMEM((dp, seqs, depth), BF16),
            pltpu.VMEM((chunks, 2, chips * seqs, chunk), F32),
            pltpu.VMEM((chunks, chips * seqs, chunk), F32),
            pltpu.VMEM((2, chunks, chips - 1, seqs, chunk // 2), jnp.int16),
            pltpu.VMEM((2, chunks, chips - 1, seqs, chunk // 2), jnp.int16),
            pltpu.VMEM((chunks, 1, spread_lanes), F32),
            pltpu.VMEM((chunks, chips - 1, 1, spread_lanes), F32),
            pltpu.VMEM((seqs, q_heads, head), F32),
            pltpu.VMEM((seqs, q_heads, head), F32),
            pltpu.VMEM((seqs, q_heads, head), F32),
            pltpu.VMEM((seqs, q_heads, head), F32),
            pltpu.VMEM((tp, 1, dp * seqs), F32),
            pltpu.VMEM((1, dp * seqs), F32),
            pltpu.VMEM((dp, seqs, LANES), F32),
            pltpu.VMEM((dp, 1, dp * seqs), F32),
            pltpu.VMEM((1, dp * seqs), F32),
            dma((6,)),
            dma((3,)),
            dma(()),
            dma(()),
            dma(()),
            dma((chunks,)),
            dma(()),
            dma((chunks + 1,)),
            dma(()),
            dma((chunks,)),
            dma(()),
            dma(()),
            dma(()),
            dma(()),
        ],
        compiler_params=pltpu.CompilerParams(
            collective_id=0, has_side_effects=True, vmem_limit_bytes=60 * 1024 * 1024
        ),
    )(
        page_table,
        lengths,
        tol_counts.reshape(1, -1),
        tokens,
        norm_gain.reshape(-1, LANES),
        check_column.reshape(-1, LANES),
        w_query,
        w_key,
        w_value,
        flat_keys,
        flat_values,
    )
    return attention, excess[0, 0]


def solution(mesh):
    return jax.shard_map(
        functools.partial(body, mesh.shape["dp"], mesh.shape["tensor"]),
        mesh=mesh,
        in_specs=(
            P("dp", None),
            P(),
            P("dp", "tensor"),
            P("dp", "tensor"),
            P("dp", "tensor"),
            P(),
            P("dp", None, "tensor", None),
            P("dp", None, "tensor", None),
            P("dp", None),
            P("dp"),
            P(),
        ),
        out_specs=(P("dp", "tensor"), P()),
        check_vma=False,
    )
```

```python
import functools
import math

import jax
import jax.numpy as jnp
from jax import lax
from jax.experimental import pallas as pl
from jax.experimental.pallas import tpu as pltpu
from jax.sharding import PartitionSpec as P

EPSILON = 1e-06
ROPE_BASE = 1000000.0
TOL_STEP = 0.25
MESH = pl.DeviceIdType.MESH
F32 = jnp.float32
BF16 = jnp.bfloat16
UNROLL = 4
LANES = 128
LEVELS = 32000.0
TINY = 1e-30
SPLIT = 3


def step_kernel(
    dp,
    tp,
    table_hbm,
    lengths_hbm,
    counts_hbm,
    tokens_hbm,
    gain_hbm,
    check_hbm,
    wq_hbm,
    wk_hbm,
    wv_hbm,
    keys_hbm,
    values_hbm,
    out_ref,
    excess_ref,
    table_ref,
    lengths_ref,
    counts_ref,
    tokens_ref,
    gain_ref,
    check_ref,
    weights,
    keys,
    values,
    key_columns,
    weight_sums,
    check_row,
    outgoing,
    spread,
    parts,
    from_pair,
    outbound,
    from_chips,
    steps_out,
    steps_in,
    queries,
    new_keys,
    new_values,
    mixed,
    sums_all,
    sums_own,
    shares,
    excess_all,
    excess_own,
    small_sems,
    load_sems,
    a2a_send,
    a2a_recv,
    pair_send,
    pair_recv,
    chip_send,
    chip_recv,
    step_send,
    step_recv,
    sum_send,
    sum_recv,
    exc_send,
    exc_recv,
):
    chips = dp // 2
    spread_lanes = steps_out.shape[2]
    me = lax.axis_index("dp")
    zed = lax.axis_index("tensor")
    chip, core = me // 2, me % 2
    seqs, width = tokens_ref.shape
    depth = width // dp
    q_width, kv_width = wq_hbm.shape[1], wk_hbm.shape[1]
    total = q_width + 2 * kv_width
    chunks, _, _, chunk = parts.shape
    head = keys_hbm.shape[2]
    q_heads, kv_heads = q_width // head, kv_width // head
    group = q_heads // kv_heads
    pages = table_ref.shape[1]
    page_rows = keys_hbm.shape[1]

    def wait_bytes(ref, sem):
        pltpu.make_async_copy(ref, ref, sem).wait()

    def partner(dc):
        other, bit = chip, 1
        while bit <= dc:
            if dc // bit % 2:
                other = other + bit - 2 * bit * (chip // bit % 2)
            bit *= 2
        return other

    def slot(q, dc):
        return (1 - q if dc else q) * chips + dc

    barrier = pltpu.get_barrier_semaphore()
    for k in range(1, dp):
        pl.semaphore_signal(
            barrier, inc=1, device_id=((me + k) % dp, zed), device_id_type=MESH
        )

    small_loads = [
        pltpu.make_async_copy(source, target, small_sems.at[i])
        for i, (source, target) in enumerate(
            [
                (tokens_hbm, tokens_ref),
                (gain_hbm, gain_ref),
                (lengths_hbm, lengths_ref),
                (table_hbm, table_ref),
                (counts_hbm, counts_ref),
                (check_hbm, check_ref),
            ]
        )
    ]
    for load in small_loads:
        load.start()
    loads = [
        pltpu.make_async_copy(keys_hbm, keys, load_sems.at[1]),
        pltpu.make_async_copy(wq_hbm, weights.at[:, pl.ds(0, q_width)], load_sems.at[0]),
        pltpu.make_async_copy(wk_hbm, weights.at[:, pl.ds(q_width, kv_width)], load_sems.at[0]),
        pltpu.make_async_copy(
            wv_hbm, weights.at[:, pl.ds(q_width + kv_width, kv_width)], load_sems.at[0]
        ),
        pltpu.make_async_copy(values_hbm, values, load_sems.at[2]),
    ]

    loads[0].start()
    for load in small_loads[:2]:
        load.wait()
    for load in loads[1:4]:
        load.start()
    square = jnp.zeros((seqs, LANES), F32)
    for j in range(width // LANES):
        part = tokens_ref[:, j * LANES : (j + 1) * LANES].astype(F32)
        square = square + part * part
    scale = lax.rsqrt(jnp.sum(square, axis=1, keepdims=True) / width + EPSILON)
    gains = gain_ref[...].astype(F32)
    for j in range(width // LANES):
        part = tokens_ref[:, j * LANES : (j + 1) * LANES].astype(F32)
        at = j * LANES % depth
        outgoing[j * LANES // depth, :, at : at + LANES] = (
            part * scale * gains[j : j + 1]
        ).astype(BF16)
    spread[0] = outgoing[me]

    pl.semaphore_wait(barrier, dp - 1 + (zed + tp - 1) // tp)

    def greet_plane(k):
        @pl.when((zed + k >= 0) & (zed + k < tp))
        def _():
            pl.semaphore_signal(barrier, inc=1, device_id=(me, zed + k), device_id_type=MESH)


    for dc in range(chips - 1, -1, -1):
        for there in range(2) if dc else [1 - core]:
            q = (there + core) % 2
            target = partner(dc) * 2 + there
            copy = pltpu.make_async_remote_copy(
                src_ref=outgoing.at[target],
                dst_ref=spread.at[slot(q, dc)],
                send_sem=a2a_send,
                recv_sem=a2a_recv,
                device_id=(target, zed),
                device_id_type=MESH,
            )
            copy.start()

    greet_plane(1)
    for k in range(1, tp):
        greet_plane(-k)

    for load in small_loads[2:5]:
        load.wait()
    seq_row = lax.broadcasted_iota(jnp.int32, (seqs, LANES), 0)
    positions = jnp.zeros((seqs, LANES), F32)
    for s in range(seqs):
        positions = jnp.where(seq_row == s, lengths_ref[s].astype(F32), positions)
    lane = lax.broadcasted_iota(jnp.int32, (seqs, head), 1)
    step = (lane % (head // 2)).astype(F32)
    angles = positions * jnp.exp(step * (-2.0 * math.log(ROPE_BASE) / head))
    cosine = jnp.cos(angles)
    sine = jnp.where(lane < head // 2, -1.0, 1.0) * jnp.sin(angles)

    near = (pages + 1) // 2
    far = pages - near
    span = near * page_rows
    no_page = jnp.zeros((page_rows, head), BF16)

    def side_by_side(pool, s):
        left = [pool[table_ref[s, p]] for p in range(near)]
        right = [pool[table_ref[s, p]] for p in range(near, pages)] + [no_page] * (near - far)
        return jnp.concatenate(
            [jnp.concatenate(left, axis=0), jnp.concatenate(right, axis=0)], axis=1
        )

    def turn_keys(s, carry):
        key_columns[s] = jnp.transpose(side_by_side(keys, s))
        return carry

    loads[0].wait()
    loads[4].start()
    lax.fori_loop(0, seqs, turn_keys, 0, unroll=UNROLL)

    small_loads[5].wait()
    checks = check_ref[...].astype(F32)
    checked = jnp.zeros((seqs, LANES), F32)
    for j in range(width // LANES):
        at = j * LANES % depth
        part = outgoing[j * LANES // depth, :, at : at + LANES].astype(F32)
        checked = checked + part * checks[j : j + 1]
    shares[...] = jnp.zeros(shares.shape, F32)
    shares[me] = jnp.where(zed == 0, checked, 0.0)
    turned_checks = jnp.transpose(shares[...].reshape(dp * seqs, LANES))
    check_row[...] = jnp.sum(turned_checks, axis=0, keepdims=True)

    wait_bytes(weights, load_sems.at[0])

    totals = lax.dot_general(
        jnp.ones((seqs, total), BF16),
        weights[...],
        (((1,), (1,)), ((), ())),
        preferred_element_type=F32,
    )
    term = lax.broadcasted_iota(jnp.int32, (seqs, depth), 0)
    split = jnp.zeros((seqs, depth), F32)
    for i in range(SPLIT):
        rounded = totals.astype(BF16).astype(F32)
        split = jnp.where(term == i, rounded, split)
        totals = totals - rounded
    weight_sums[...] = split.astype(BF16)

    wait_bytes(spread.at[pl.ds(1, dp - 1)], a2a_recv)

    pair_copies = []
    batch = seqs // 2
    half = chips * seqs

    def project(c):
        product = jnp.dot(
            spread[...].reshape(dp * seqs, depth),
            weights[:, pl.ds(c * chunk, chunk)],
            preferred_element_type=F32,
        )
        parts[c, 1] = product[half:]
        copy = pltpu.make_async_remote_copy(
            src_ref=parts.at[c, 1],
            dst_ref=from_pair.at[c],
            send_sem=pair_send,
            recv_sem=pair_recv.at[c],
            device_id=(chip * 2 + (core + 1) % 2, zed),
            device_id_type=MESH,
        )
        copy.start()
        pair_copies.append(copy)
        parts[c, 0] = product[:half]

    spots = lax.broadcasted_iota(jnp.int32, (half - seqs, spread_lanes), 1)
    spot_rows = lax.broadcasted_iota(jnp.int32, (half - seqs, spread_lanes), 0)

    def pass_on(c):
        pair_copies[c].wait_recv()
        summed = parts[c, 0, pl.ds(seqs, half - seqs)] + from_pair[c, pl.ds(seqs, half - seqs)]
        largest = jnp.max(jnp.abs(summed), axis=1, keepdims=True)
        step = (jnp.maximum(largest, TINY) * (1.0 / LEVELS)).astype(BF16).astype(F32)
        coded = jnp.round(summed * (1.0 / step)).astype(jnp.int32)
        for dc in range(1, chips):
            for h in range(2):
                at = (dc - 1) * seqs + h * batch
                stacked = jnp.concatenate(
                    [coded[at : at + batch, : chunk // 2], coded[at : at + batch, chunk // 2 :]],
                    axis=0,
                )
                outbound[h, c, dc - 1] = stacked.astype(jnp.int16)
        steps_out[c] = jnp.sum(jnp.where(spots == spot_rows, step, 0.0), axis=0, keepdims=True)
        for dc in range(chips - 1, 0, -1):
            send_on(steps_out.at[c], steps_in.at[c, dc - 1], step_send, step_recv.at[c], dc)
        send_batch(0, c)

    def send_batch(h, c):
        for dc in range(chips - 1, 0, -1):
            send_on(
                outbound.at[h, c, dc - 1],
                from_chips.at[h, c, dc - 1],
                chip_send,
                chip_recv.at[c if h == 0 else chunks],
                dc,
            )

    def send_on(source, target, send_sem, recv_sem, dc):
        pltpu.make_async_remote_copy(
            src_ref=source,
            dst_ref=target,
            send_sem=send_sem,
            recv_sem=recv_sem,
            device_id=(partner(dc) * 2 + (core + 1) % 2, zed),
            device_id_type=MESH,
        ).start()

    def exchange(own, everyone, place, targets, send_sem, recv_sem):
        everyone[place] = own[...]
        for target in targets:
            pltpu.make_async_remote_copy(
                src_ref=own,
                dst_ref=everyone.at[place],
                send_sem=send_sem,
                recv_sem=recv_sem,
                device_id=target,
                device_id_type=MESH,
            ).start()

    def send_sums():
        blocks = []
        for owner in range(dp):
            there = owner // 2
            relative, bit = 0, 1
            while bit < chips:
                mine, other = chip // bit % 2, there // bit % 2
                relative = relative + bit * ((mine + other) % 2)
                bit *= 2
            kept = (core + owner + (relative + chips - 1) // chips) % 2
            blocks.append(spread[kept * chips + relative])
        terms = lax.dot_general(
            weight_sums[...],
            jnp.concatenate(blocks, axis=0),
            (((1,), (1,)), ((), ())),
            preferred_element_type=F32,
        )
        excess_own[...] = jnp.sum(terms, axis=0, keepdims=True) - check_row[...]
        exchange(
            excess_own, excess_all, me, [((me + k) % dp, zed) for k in range(1, dp)], exc_send, exc_recv
        )

    for c in range(chunks):
        project(c)
        if c == 0:
            send_sums()
        if c >= 3:
            pass_on(c - 3)
    for c in range(max(chunks - 3, 0), chunks):
        pass_on(c)
    for c in range(chunks):
        send_batch(1, c)

    def finish_group():
        wait_bytes(excess_all.at[pl.ds(1, dp - 1)], exc_recv)
        group_sum = excess_all[0]
        for k in range(1, dp):
            group_sum = group_sum + excess_all[k]
        sums_own[...] = group_sum

        @pl.when(zed < tp - 1)
        def _():
            pl.semaphore_wait(barrier, tp - 1 - zed)

        exchange(
            sums_own, sums_all, zed, [(me, (zed + k) % tp) for k in range(1, tp)], sum_send, sum_recv
        )

    def rotate(vector, rows):
        return (
            (vector * cosine[rows] + pltpu.roll(vector, head // 2, 1) * sine[rows])
            .astype(BF16)
            .astype(F32)
        )

    def settle(h, c):
        if h == 0:
            wait_bytes(steps_in.at[c], step_recv.at[c])
            wait_bytes(from_chips.at[h, c], chip_recv.at[c])
        rows = slice(h * batch, (h + 1) * batch)
        own = parts[c, 0, rows] + from_pair[c, rows]
        for dc in range(1, chips):
            spot = spot_rows[rows] + (dc - 1) * seqs
            step = jnp.sum(
                jnp.where(spots[rows] == spot, steps_in[c, dc - 1], 0.0), axis=1, keepdims=True
            )
            stacked = from_chips[h, c, dc - 1].astype(jnp.int32).astype(F32)
            own = own + jnp.concatenate([stacked[:batch], stacked[batch:]], axis=1) * step
        for i in range(chunk // head):
            block = own[:, i * head : (i + 1) * head]
            index = c * (chunk // head) + i
            if index < q_heads:
                queries[rows, index, :] = rotate(block, rows)
            elif index < q_heads + kv_heads:
                k = index - q_heads
                turned = rotate(block, rows)
                for g in range(group):
                    new_keys[rows, k * group + g, :] = turned
            else:
                k = index - q_heads - kv_heads
                rounded = block.astype(BF16).astype(F32)
                for g in range(group):
                    new_values[rows, k * group + g, :] = rounded

    column = lax.broadcasted_iota(jnp.int32, (2 * q_heads, span), 1)
    row = lax.broadcasted_iota(jnp.int32, (2 * q_heads, span), 0)
    place = jnp.where(
        column % kv_heads == row % q_heads // group,
        column // kv_heads + row // q_heads * (span // kv_heads),
        pages * page_rows,
    )
    score_scale = head ** (-0.5)
    no_query = jnp.zeros((q_heads, head), BF16)
    loads[4].wait()

    def one_sequence(s):
        query = queries[s]
        narrow = query.astype(BF16)
        paired = jnp.concatenate(
            [
                jnp.concatenate([narrow, no_query], axis=1),
                jnp.concatenate([no_query, narrow], axis=1),
            ],
            axis=0,
        )
        scores = jnp.dot(paired, key_columns[s], preferred_element_type=F32) * score_scale
        new_score = jnp.sum(query * new_keys[s], axis=1, keepdims=True) * score_scale
        masked = jnp.where(place < lengths_ref[s], scores, -jnp.inf)
        highest = jnp.max(masked, axis=1, keepdims=True)
        peak = jnp.maximum(jnp.maximum(highest[:q_heads], highest[q_heads:]), new_score)
        soft = jnp.exp(masked - jnp.concatenate([peak, peak], axis=0))
        new_weight = jnp.exp(new_score - peak)
        sums = jnp.sum(soft, axis=1, keepdims=True)
        denominator = sums[:q_heads] + sums[q_heads:] + new_weight
        result = jnp.dot(
            soft.astype(BF16), side_by_side(values, s), preferred_element_type=F32
        )
        result = result[:q_heads, :head] + result[q_heads:, head:]
        result = result + new_weight.astype(BF16).astype(F32) * new_values[s]
        mixed[s] = result / denominator

    for h in range(2):
        if h == 0:
            finish_group()
        else:
            wait_bytes(from_chips.at[1], chip_recv.at[chunks])
        for c in range(chunks):
            settle(h, c)
        for s in range(h * batch, (h + 1) * batch):
            one_sequence(s)
        rows = slice(h * batch, (h + 1) * batch)
        for i in range(q_heads):
            out_ref[rows, i * head : (i + 1) * head] = mixed[rows, i, :].astype(BF16)

    wait_bytes(sums_all.at[pl.ds(1, tp - 1)], sum_recv)
    grand = sums_all[0]
    for k in range(1, tp):
        grand = grand + sums_all[k]
    residual = grand / math.sqrt(total * tp)
    over = jnp.maximum(jnp.abs(residual) - TOL_STEP * counts_ref[...].astype(F32), 0.0)
    excess_ref[...] = jnp.broadcast_to(
        jnp.sum(over, axis=1, keepdims=True) / math.sqrt(seqs * dp), excess_ref.shape
    )

    wait_bytes(spread.at[pl.ds(1, dp - 1)], a2a_send)
    wait_bytes(from_pair, pair_send)
    wait_bytes(from_chips, chip_send)
    wait_bytes(steps_in, step_send)
    wait_bytes(sums_all.at[pl.ds(1, tp - 1)], sum_send)
    wait_bytes(excess_all.at[pl.ds(1, dp - 1)], exc_send)


def hand_out(attention, excess, attention_out, excess_out, single, sems):
    first = pltpu.make_async_copy(attention, attention_out, sems.at[0])
    first.start()
    single[...] = excess[0:1, 0:1]
    second = pltpu.make_async_copy(single, excess_out, sems.at[1])
    second.start()
    first.wait()
    second.wait()


def body(
    dp,
    tp,
    tokens,
    norm_gain,
    w_query,
    w_key,
    w_value,
    check_column,
    key_cache,
    value_cache,
    page_table,
    lengths,
    tol_counts,
):
    seqs, width = tokens.shape
    head = key_cache.shape[-1]
    q_width, kv_width = w_query.shape[1], w_key.shape[1]
    total = q_width + 2 * kv_width
    q_heads = q_width // head
    depth = width // dp
    chips = dp // 2
    chunks = 5 if total % (5 * head) == 0 else 1
    chunk = total // chunks
    spread_lanes = -(-(chips - 1) * seqs // LANES) * LANES
    flat_keys = key_cache.reshape(key_cache.shape[0], -1, head)
    flat_values = value_cache.reshape(value_cache.shape[0], -1, head)

    vmem = pl.BlockSpec(memory_space=pltpu.VMEM)
    hbm = pl.BlockSpec(memory_space=pltpu.HBM)
    dma = pltpu.SemaphoreType.DMA
    attention, excess = pl.pallas_call(
        functools.partial(step_kernel, dp, tp),
        out_shape=(
            pltpu.VMEM((seqs, q_width), BF16),
            pltpu.VMEM((8, LANES), F32),
        ),
        in_specs=[hbm] * 11,
        out_specs=(vmem, vmem),
        scratch_shapes=[
            pltpu.SMEM(page_table.shape, jnp.int32),
            pltpu.SMEM(lengths.shape, jnp.int32),
            pltpu.VMEM((1, tol_counts.shape[0]), jnp.int32),
            pltpu.VMEM(tokens.shape, BF16),
            pltpu.VMEM((width // LANES, LANES), BF16),
            pltpu.VMEM((width // LANES, LANES), BF16),
            pltpu.VMEM((depth, total), BF16),
            pltpu.VMEM(flat_keys.shape, BF16),
            pltpu.VMEM(flat_values.shape, BF16),
            pltpu.VMEM((seqs, 2 * head, (page_table.shape[1] + 1) // 2 * flat_keys.shape[1]), BF16),
            pltpu.VMEM((seqs, depth), BF16),
            pltpu.VMEM((1, dp * seqs), F32),
            pltpu.VMEM((dp, seqs, depth), BF16),
            pltpu.VMEM((dp, seqs, depth), BF16),
            pltpu.VMEM((chunks, 2, chips * seqs, chunk), F32),
            pltpu.VMEM((chunks, chips * seqs, chunk), F32),
            pltpu.VMEM((2, chunks, chips - 1, seqs, chunk // 2), jnp.int16),
            pltpu.VMEM((2, chunks, chips - 1, seqs, chunk // 2), jnp.int16),
            pltpu.VMEM((chunks, 1, spread_lanes), F32),
            pltpu.VMEM((chunks, chips - 1, 1, spread_lanes), F32),
            pltpu.VMEM((seqs, q_heads, head), F32),
            pltpu.VMEM((seqs, q_heads, head), F32),
            pltpu.VMEM((seqs, q_heads, head), F32),
            pltpu.VMEM((seqs, q_heads, head), F32),
            pltpu.VMEM((tp, 1, dp * seqs), F32),
            pltpu.VMEM((1, dp * seqs), F32),
            pltpu.VMEM((dp, seqs, LANES), F32),
            pltpu.VMEM((dp, 1, dp * seqs), F32),
            pltpu.VMEM((1, dp * seqs), F32),
            dma((6,)),
            dma((3,)),
            dma(()),
            dma(()),
            dma(()),
            dma((chunks,)),
            dma(()),
            dma((chunks + 1,)),
            dma(()),
            dma((chunks,)),
            dma(()),
            dma(()),
            dma(()),
            dma(()),
        ],
        compiler_params=pltpu.CompilerParams(
            collective_id=0, has_side_effects=True, vmem_limit_bytes=60 * 1024 * 1024
        ),
    )(
        page_table,
        lengths,
        tol_counts.reshape(1, -1),
        tokens,
        norm_gain.reshape(-1, LANES),
        check_column.reshape(-1, LANES),
        w_query,
        w_key,
        w_value,
        flat_keys,
        flat_values,
    )
    attention, excess = pl.pallas_call(
        hand_out,
        out_shape=(
            jax.ShapeDtypeStruct((seqs, q_width), BF16),
            jax.ShapeDtypeStruct((1, 1), F32),
        ),
        in_specs=[vmem, vmem],
        out_specs=(hbm, hbm),
        scratch_shapes=[pltpu.VMEM((1, 1), F32), dma((2,))],
    )(
        pltpu.with_memory_space_constraint(attention, pltpu.VMEM),
        pltpu.with_memory_space_constraint(excess, pltpu.VMEM),
    )
    return attention, excess[0, 0]


def solution(mesh):
    return jax.shard_map(
        functools.partial(body, mesh.shape["dp"], mesh.shape["tensor"]),
        mesh=mesh,
        in_specs=(
            P("dp", None),
            P(),
            P("dp", "tensor"),
            P("dp", "tensor"),
            P("dp", "tensor"),
            P(),
            P("dp", None, "tensor", None),
            P("dp", None, "tensor", None),
            P("dp", None),
            P("dp"),
            P(),
        ),
        out_specs=(P("dp", "tensor"), P()),
        check_vma=False,
    )
```

```python
import functools
import math

import jax
import jax.numpy as jnp
from jax import lax
from jax.experimental import pallas as pl
from jax.experimental.pallas import tpu as pltpu
from jax.sharding import PartitionSpec as P

EPSILON = 1e-06
ROPE_BASE = 1000000.0
TOL_STEP = 0.25
MESH = pl.DeviceIdType.MESH
F32 = jnp.float32
BF16 = jnp.bfloat16
UNROLL = 4
LANES = 128
LEVELS = 32000.0
TINY = 1e-30
SPLIT = 3


def step_kernel(
    dp,
    tp,
    table_hbm,
    lengths_hbm,
    counts_hbm,
    tokens_hbm,
    gain_hbm,
    check_hbm,
    wq_hbm,
    wk_hbm,
    wv_hbm,
    keys_hbm,
    values_hbm,
    out_ref,
    excess_ref,
    table_ref,
    lengths_ref,
    counts_ref,
    tokens_ref,
    gain_ref,
    check_ref,
    weights,
    keys,
    values,
    key_columns,
    weight_sums,
    check_row,
    outgoing,
    spread,
    parts,
    from_pair,
    outbound,
    from_chips,
    steps_out,
    steps_in,
    queries,
    new_keys,
    new_values,
    mixed,
    sums_all,
    sums_own,
    shares,
    excess_all,
    excess_own,
    small_sems,
    load_sems,
    a2a_send,
    a2a_recv,
    pair_send,
    pair_recv,
    chip_send,
    chip_recv,
    step_send,
    step_recv,
    sum_send,
    sum_recv,
    exc_send,
    exc_recv,
):
    chips = dp // 2
    spread_lanes = steps_out.shape[2]
    me = lax.axis_index("dp")
    zed = lax.axis_index("tensor")
    chip, core = me // 2, me % 2
    seqs, width = tokens_ref.shape
    depth = width // dp
    q_width, kv_width = wq_hbm.shape[1], wk_hbm.shape[1]
    total = q_width + 2 * kv_width
    chunks, _, _, chunk = parts.shape
    head = keys_hbm.shape[2]
    q_heads, kv_heads = q_width // head, kv_width // head
    group = q_heads // kv_heads
    pages = table_ref.shape[1]
    page_rows = keys_hbm.shape[1]

    def wait_bytes(ref, sem):
        pltpu.make_async_copy(ref, ref, sem).wait()

    def partner(dc):
        other, bit = chip, 1
        while bit <= dc:
            if dc // bit % 2:
                other = other + bit - 2 * bit * (chip // bit % 2)
            bit *= 2
        return other

    def slot(q, dc):
        return (1 - q if dc else q) * chips + dc

    barrier = pltpu.get_barrier_semaphore()
    for k in range(1, dp):
        pl.semaphore_signal(
            barrier, inc=1, device_id=((me + k) % dp, zed), device_id_type=MESH
        )

    small_loads = [
        pltpu.make_async_copy(source, target, small_sems.at[i])
        for i, (source, target) in enumerate(
            [
                (tokens_hbm, tokens_ref),
                (gain_hbm, gain_ref),
                (lengths_hbm, lengths_ref),
                (table_hbm, table_ref),
                (counts_hbm, counts_ref),
                (check_hbm, check_ref),
            ]
        )
    ]
    for load in small_loads:
        load.start()
    loads = [
        pltpu.make_async_copy(keys_hbm, keys, load_sems.at[1]),
        pltpu.make_async_copy(wq_hbm, weights.at[:, pl.ds(0, q_width)], load_sems.at[0]),
        pltpu.make_async_copy(wk_hbm, weights.at[:, pl.ds(q_width, kv_width)], load_sems.at[0]),
        pltpu.make_async_copy(
            wv_hbm, weights.at[:, pl.ds(q_width + kv_width, kv_width)], load_sems.at[0]
        ),
        pltpu.make_async_copy(values_hbm, values, load_sems.at[2]),
    ]

    loads[0].start()
    for load in small_loads[:2]:
        load.wait()
    for load in loads[1:4]:
        load.start()
    square = jnp.zeros((seqs, LANES), F32)
    for j in range(width // LANES):
        part = tokens_ref[:, j * LANES : (j + 1) * LANES].astype(F32)
        square = square + part * part
    scale = lax.rsqrt(jnp.sum(square, axis=1, keepdims=True) / width + EPSILON)
    gains = gain_ref[...].astype(F32)
    for j in range(width // LANES):
        part = tokens_ref[:, j * LANES : (j + 1) * LANES].astype(F32)
        at = j * LANES % depth
        outgoing[j * LANES // depth, :, at : at + LANES] = (
            part * scale * gains[j : j + 1]
        ).astype(BF16)
    spread[0] = outgoing[me]

    pl.semaphore_wait(barrier, dp - 1 + (zed + tp - 1) // tp)

    def greet_plane(k):
        @pl.when((zed + k >= 0) & (zed + k < tp))
        def _():
            pl.semaphore_signal(barrier, inc=1, device_id=(me, zed + k), device_id_type=MESH)


    for dc in range(chips - 1, -1, -1):
        for there in range(2) if dc else [1 - core]:
            q = (there + core) % 2
            target = partner(dc) * 2 + there
            copy = pltpu.make_async_remote_copy(
                src_ref=outgoing.at[target],
                dst_ref=spread.at[slot(q, dc)],
                send_sem=a2a_send,
                recv_sem=a2a_recv,
                device_id=(target, zed),
                device_id_type=MESH,
            )
            copy.start()

    greet_plane(1)
    for k in range(1, tp):
        greet_plane(-k)

    for load in small_loads[2:5]:
        load.wait()
    seq_row = lax.broadcasted_iota(jnp.int32, (seqs, LANES), 0)
    positions = jnp.zeros((seqs, LANES), F32)
    for s in range(seqs):
        positions = jnp.where(seq_row == s, lengths_ref[s].astype(F32), positions)
    lane = lax.broadcasted_iota(jnp.int32, (seqs, head), 1)
    step = (lane % (head // 2)).astype(F32)
    angles = positions * jnp.exp(step * (-2.0 * math.log(ROPE_BASE) / head))
    cosine = jnp.cos(angles)
    sine = jnp.where(lane < head // 2, -1.0, 1.0) * jnp.sin(angles)

    near = (pages + 1) // 2
    far = pages - near
    span = near * page_rows
    no_page = jnp.zeros((page_rows, head), BF16)

    def side_by_side(pool, s):
        left = [pool[table_ref[s, p]] for p in range(near)]
        right = [pool[table_ref[s, p]] for p in range(near, pages)] + [no_page] * (near - far)
        return jnp.concatenate(
            [jnp.concatenate(left, axis=0), jnp.concatenate(right, axis=0)], axis=1
        )

    def turn_keys(s, carry):
        key_columns[s] = jnp.transpose(side_by_side(keys, s))
        return carry

    loads[0].wait()
    loads[4].start()
    lax.fori_loop(0, seqs, turn_keys, 0, unroll=UNROLL)

    small_loads[5].wait()
    checks = check_ref[...].astype(F32)
    checked = jnp.zeros((seqs, LANES), F32)
    for j in range(width // LANES):
        at = j * LANES % depth
        part = outgoing[j * LANES // depth, :, at : at + LANES].astype(F32)
        checked = checked + part * checks[j : j + 1]
    shares[...] = jnp.zeros(shares.shape, F32)
    shares[me] = jnp.where(zed == 0, checked, 0.0)
    turned_checks = jnp.transpose(shares[...].reshape(dp * seqs, LANES))
    check_row[...] = jnp.sum(turned_checks, axis=0, keepdims=True)

    wait_bytes(weights, load_sems.at[0])

    totals = lax.dot_general(
        jnp.ones((seqs, total), BF16),
        weights[...],
        (((1,), (1,)), ((), ())),
        preferred_element_type=F32,
    )
    term = lax.broadcasted_iota(jnp.int32, (seqs, depth), 0)
    split = jnp.zeros((seqs, depth), F32)
    for i in range(SPLIT):
        rounded = totals.astype(BF16).astype(F32)
        split = jnp.where(term == i, rounded, split)
        totals = totals - rounded
    weight_sums[...] = split.astype(BF16)

    wait_bytes(spread.at[pl.ds(1, dp - 1)], a2a_recv)

    pair_copies = []
    middle = (chunks + 1) // 2
    step_groups = [(0, middle)] + [(middle, chunks)] * (chunks > 1)
    batch = seqs // 2
    half = chips * seqs

    def project(c):
        product = jnp.dot(
            spread[...].reshape(dp * seqs, depth),
            weights[:, pl.ds(c * chunk, chunk)],
            preferred_element_type=F32,
        )
        parts[c, 1] = product[half:]
        copy = pltpu.make_async_remote_copy(
            src_ref=parts.at[c, 1],
            dst_ref=from_pair.at[c],
            send_sem=pair_send,
            recv_sem=pair_recv.at[c],
            device_id=(chip * 2 + (core + 1) % 2, zed),
            device_id_type=MESH,
        )
        copy.start()
        pair_copies.append(copy)
        parts[c, 0] = product[:half]

    spots = lax.broadcasted_iota(jnp.int32, (half - seqs, spread_lanes), 1)
    spot_rows = lax.broadcasted_iota(jnp.int32, (half - seqs, spread_lanes), 0)

    def pass_on(c):
        pair_copies[c].wait_recv()
        summed = parts[c, 0, pl.ds(seqs, half - seqs)] + from_pair[c, pl.ds(seqs, half - seqs)]
        largest = jnp.max(jnp.abs(summed), axis=1, keepdims=True)
        step = (jnp.maximum(largest, TINY) * (1.0 / LEVELS)).astype(BF16).astype(F32)
        coded = jnp.round(summed * (1.0 / step)).astype(jnp.int32)
        for dc in range(1, chips):
            for h in range(2):
                at = (dc - 1) * seqs + h * batch
                stacked = jnp.concatenate(
                    [coded[at : at + batch, : chunk // 2], coded[at : at + batch, chunk // 2 :]],
                    axis=0,
                )
                outbound[h, c, dc - 1] = stacked.astype(jnp.int16)
        steps_out[c] = jnp.sum(jnp.where(spots == spot_rows, step, 0.0), axis=0, keepdims=True)
        for g, (first, last) in enumerate(step_groups):
            if c == last - 1:
                some = pl.ds(first, last - first)
                for dc in range(chips - 1, 0, -1):
                    send_on(
                        steps_out.at[some],
                        steps_in.at[dc - 1, some],
                        step_send,
                        step_recv.at[g],
                        dc,
                    )
        send_batch(0, c)

    def send_batch(h, c):
        for dc in range(chips - 1, 0, -1):
            send_on(
                outbound.at[h, c, dc - 1],
                from_chips.at[h, c, dc - 1],
                chip_send,
                chip_recv.at[c if h == 0 else chunks],
                dc,
            )

    def send_on(source, target, send_sem, recv_sem, dc):
        pltpu.make_async_remote_copy(
            src_ref=source,
            dst_ref=target,
            send_sem=send_sem,
            recv_sem=recv_sem,
            device_id=(partner(dc) * 2 + (core + 1) % 2, zed),
            device_id_type=MESH,
        ).start()

    def exchange(own, everyone, place, targets, send_sem, recv_sem):
        everyone[place] = own[...]
        for target in targets:
            pltpu.make_async_remote_copy(
                src_ref=own,
                dst_ref=everyone.at[place],
                send_sem=send_sem,
                recv_sem=recv_sem,
                device_id=target,
                device_id_type=MESH,
            ).start()

    def add_sums():
        blocks = []
        for owner in range(dp):
            there = owner // 2
            relative, bit = 0, 1
            while bit < chips:
                mine, other = chip // bit % 2, there // bit % 2
                relative = relative + bit * ((mine + other) % 2)
                bit *= 2
            kept = (core + owner + (relative + chips - 1) // chips) % 2
            blocks.append(spread[kept * chips + relative])
        terms = lax.dot_general(
            weight_sums[...],
            jnp.concatenate(blocks, axis=0),
            (((1,), (1,)), ((), ())),
            preferred_element_type=F32,
        )
        excess_own[...] = jnp.sum(terms, axis=0, keepdims=True) - check_row[...]

    def send_sums():
        exchange(
            excess_own, excess_all, me, [((me + k) % dp, zed) for k in range(1, dp)], exc_send, exc_recv
        )

    add_sums()
    for c in range(chunks):
        project(c)
        if c == 0:
            send_sums()
        if c >= 3:
            pass_on(c - 3)
    for c in range(max(chunks - 3, 0), chunks):
        pass_on(c)
    for c in range(chunks):
        send_batch(1, c)

    def finish_group():
        wait_bytes(excess_all.at[pl.ds(1, dp - 1)], exc_recv)
        group_sum = excess_all[0]
        for k in range(1, dp):
            group_sum = group_sum + excess_all[k]
        sums_own[...] = group_sum

        @pl.when(zed < tp - 1)
        def _():
            pl.semaphore_wait(barrier, tp - 1 - zed)

        exchange(
            sums_own, sums_all, zed, [(me, (zed + k) % tp) for k in range(1, tp)], sum_send, sum_recv
        )

    def rotate(vector, rows):
        return (
            (vector * cosine[rows] + pltpu.roll(vector, head // 2, 1) * sine[rows])
            .astype(BF16)
            .astype(F32)
        )

    def settle(h, c):
        if h == 0:
            for g, (first, last) in enumerate(step_groups):
                if c == first:
                    some = pl.ds(first, last - first)
                    wait_bytes(steps_in.at[:, some], step_recv.at[g])
            wait_bytes(from_chips.at[h, c], chip_recv.at[c])
        rows = slice(h * batch, (h + 1) * batch)
        own = parts[c, 0, rows] + from_pair[c, rows]
        for dc in range(1, chips):
            spot = spot_rows[rows] + (dc - 1) * seqs
            step = jnp.sum(
                jnp.where(spots[rows] == spot, steps_in[dc - 1, c], 0.0), axis=1, keepdims=True
            )
            stacked = from_chips[h, c, dc - 1].astype(jnp.int32).astype(F32)
            own = own + jnp.concatenate([stacked[:batch], stacked[batch:]], axis=1) * step
        for i in range(chunk // head):
            block = own[:, i * head : (i + 1) * head]
            index = c * (chunk // head) + i
            if index < q_heads:
                queries[rows, index, :] = rotate(block, rows)
            elif index < q_heads + kv_heads:
                k = index - q_heads
                turned = rotate(block, rows)
                for g in range(group):
                    new_keys[rows, k * group + g, :] = turned
            else:
                k = index - q_heads - kv_heads
                rounded = block.astype(BF16).astype(F32)
                for g in range(group):
                    new_values[rows, k * group + g, :] = rounded

    column = lax.broadcasted_iota(jnp.int32, (2 * q_heads, span), 1)
    row = lax.broadcasted_iota(jnp.int32, (2 * q_heads, span), 0)
    place = jnp.where(
        column % kv_heads == row % q_heads // group,
        column // kv_heads + row // q_heads * (span // kv_heads),
        pages * page_rows,
    )
    score_scale = head ** (-0.5)
    no_query = jnp.zeros((q_heads, head), BF16)
    loads[4].wait()

    def one_sequence(s):
        query = queries[s]
        narrow = query.astype(BF16)
        paired = jnp.concatenate(
            [
                jnp.concatenate([narrow, no_query], axis=1),
                jnp.concatenate([no_query, narrow], axis=1),
            ],
            axis=0,
        )
        scores = jnp.dot(paired, key_columns[s], preferred_element_type=F32) * score_scale
        new_score = jnp.sum(query * new_keys[s], axis=1, keepdims=True) * score_scale
        masked = jnp.where(place < lengths_ref[s], scores, -jnp.inf)
        highest = jnp.max(masked, axis=1, keepdims=True)
        peak = jnp.maximum(jnp.maximum(highest[:q_heads], highest[q_heads:]), new_score)
        soft = jnp.exp(masked - jnp.concatenate([peak, peak], axis=0))
        new_weight = jnp.exp(new_score - peak)
        sums = jnp.sum(soft, axis=1, keepdims=True)
        denominator = sums[:q_heads] + sums[q_heads:] + new_weight
        result = jnp.dot(
            soft.astype(BF16), side_by_side(values, s), preferred_element_type=F32
        )
        result = result[:q_heads, :head] + result[q_heads:, head:]
        result = result + new_weight.astype(BF16).astype(F32) * new_values[s]
        mixed[s] = result / denominator

    for h in range(2):
        if h == 0:
            finish_group()
        else:
            wait_bytes(from_chips.at[1], chip_recv.at[chunks])
        for c in range(chunks):
            settle(h, c)
        for s in range(h * batch, (h + 1) * batch):
            one_sequence(s)
        rows = slice(h * batch, (h + 1) * batch)
        for i in range(q_heads):
            out_ref[rows, i * head : (i + 1) * head] = mixed[rows, i, :].astype(BF16)

    wait_bytes(sums_all.at[pl.ds(1, tp - 1)], sum_recv)
    grand = sums_all[0]
    for k in range(1, tp):
        grand = grand + sums_all[k]
    residual = grand / math.sqrt(total * tp)
    over = jnp.maximum(jnp.abs(residual) - TOL_STEP * counts_ref[...].astype(F32), 0.0)
    excess_ref[...] = jnp.broadcast_to(
        jnp.sum(over, axis=1, keepdims=True) / math.sqrt(seqs * dp), excess_ref.shape
    )

    wait_bytes(spread.at[pl.ds(1, dp - 1)], a2a_send)
    wait_bytes(from_pair, pair_send)
    wait_bytes(from_chips, chip_send)
    wait_bytes(steps_in, step_send)
    wait_bytes(sums_all.at[pl.ds(1, tp - 1)], sum_send)
    wait_bytes(excess_all.at[pl.ds(1, dp - 1)], exc_send)


def hand_out(attention, excess, attention_out, excess_out, single, sems):
    first = pltpu.make_async_copy(attention, attention_out, sems.at[0])
    first.start()
    single[...] = excess[0:1, 0:1]
    second = pltpu.make_async_copy(single, excess_out, sems.at[1])
    second.start()
    first.wait()
    second.wait()


def body(
    dp,
    tp,
    tokens,
    norm_gain,
    w_query,
    w_key,
    w_value,
    check_column,
    key_cache,
    value_cache,
    page_table,
    lengths,
    tol_counts,
):
    seqs, width = tokens.shape
    head = key_cache.shape[-1]
    q_width, kv_width = w_query.shape[1], w_key.shape[1]
    total = q_width + 2 * kv_width
    q_heads = q_width // head
    depth = width // dp
    chips = dp // 2
    chunks = 5 if total % (5 * head) == 0 else 1
    chunk = total // chunks
    spread_lanes = -(-(chips - 1) * seqs // LANES) * LANES
    flat_keys = key_cache.reshape(key_cache.shape[0], -1, head)
    flat_values = value_cache.reshape(value_cache.shape[0], -1, head)

    vmem = pl.BlockSpec(memory_space=pltpu.VMEM)
    hbm = pl.BlockSpec(memory_space=pltpu.HBM)
    dma = pltpu.SemaphoreType.DMA
    attention, excess = pl.pallas_call(
        functools.partial(step_kernel, dp, tp),
        out_shape=(
            pltpu.VMEM((seqs, q_width), BF16),
            pltpu.VMEM((8, LANES), F32),
        ),
        in_specs=[hbm] * 11,
        out_specs=(vmem, vmem),
        scratch_shapes=[
            pltpu.SMEM(page_table.shape, jnp.int32),
            pltpu.SMEM(lengths.shape, jnp.int32),
            pltpu.VMEM((1, tol_counts.shape[0]), jnp.int32),
            pltpu.VMEM(tokens.shape, BF16),
            pltpu.VMEM((width // LANES, LANES), BF16),
            pltpu.VMEM((width // LANES, LANES), BF16),
            pltpu.VMEM((depth, total), BF16),
            pltpu.VMEM(flat_keys.shape, BF16),
            pltpu.VMEM(flat_values.shape, BF16),
            pltpu.VMEM((seqs, 2 * head, (page_table.shape[1] + 1) // 2 * flat_keys.shape[1]), BF16),
            pltpu.VMEM((seqs, depth), BF16),
            pltpu.VMEM((1, dp * seqs), F32),
            pltpu.VMEM((dp, seqs, depth), BF16),
            pltpu.VMEM((dp, seqs, depth), BF16),
            pltpu.VMEM((chunks, 2, chips * seqs, chunk), F32),
            pltpu.VMEM((chunks, chips * seqs, chunk), F32),
            pltpu.VMEM((2, chunks, chips - 1, seqs, chunk // 2), jnp.int16),
            pltpu.VMEM((2, chunks, chips - 1, seqs, chunk // 2), jnp.int16),
            pltpu.VMEM((chunks, 1, spread_lanes), F32),
            pltpu.VMEM((chips - 1, chunks, 1, spread_lanes), F32),
            pltpu.VMEM((seqs, q_heads, head), F32),
            pltpu.VMEM((seqs, q_heads, head), F32),
            pltpu.VMEM((seqs, q_heads, head), F32),
            pltpu.VMEM((seqs, q_heads, head), F32),
            pltpu.VMEM((tp, 1, dp * seqs), F32),
            pltpu.VMEM((1, dp * seqs), F32),
            pltpu.VMEM((dp, seqs, LANES), F32),
            pltpu.VMEM((dp, 1, dp * seqs), F32),
            pltpu.VMEM((1, dp * seqs), F32),
            dma((6,)),
            dma((3,)),
            dma(()),
            dma(()),
            dma(()),
            dma((chunks,)),
            dma(()),
            dma((chunks + 1,)),
            dma(()),
            dma((2,)),
            dma(()),
            dma(()),
            dma(()),
            dma(()),
        ],
        compiler_params=pltpu.CompilerParams(
            collective_id=0, has_side_effects=True, vmem_limit_bytes=60 * 1024 * 1024
        ),
    )(
        page_table,
        lengths,
        tol_counts.reshape(1, -1),
        tokens,
        norm_gain.reshape(-1, LANES),
        check_column.reshape(-1, LANES),
        w_query,
        w_key,
        w_value,
        flat_keys,
        flat_values,
    )
    attention, excess = pl.pallas_call(
        hand_out,
        out_shape=(
            jax.ShapeDtypeStruct((seqs, q_width), BF16),
            jax.ShapeDtypeStruct((1, 1), F32),
        ),
        in_specs=[vmem, vmem],
        out_specs=(hbm, hbm),
        scratch_shapes=[pltpu.VMEM((1, 1), F32), dma((2,))],
    )(
        pltpu.with_memory_space_constraint(attention, pltpu.VMEM),
        pltpu.with_memory_space_constraint(excess, pltpu.VMEM),
    )
    return attention, excess[0, 0]


def solution(mesh):
    return jax.shard_map(
        functools.partial(body, mesh.shape["dp"], mesh.shape["tensor"]),
        mesh=mesh,
        in_specs=(
            P("dp", None),
            P(),
            P("dp", "tensor"),
            P("dp", "tensor"),
            P("dp", "tensor"),
            P(),
            P("dp", None, "tensor", None),
            P("dp", None, "tensor", None),
            P("dp", None),
            P("dp"),
            P(),
        ),
        out_specs=(P("dp", "tensor"), P()),
        check_vma=False,
    )
```

```python
import functools
import math

import jax
import jax.numpy as jnp
from jax import lax
from jax.experimental import pallas as pl
from jax.experimental.pallas import tpu as pltpu
from jax.sharding import PartitionSpec as P

EPSILON = 1e-06
ROPE_BASE = 1000000.0
TOL_STEP = 0.25
MESH = pl.DeviceIdType.MESH
F32 = jnp.float32
BF16 = jnp.bfloat16
UNROLL = 4
LANES = 128
LEVELS = 32000.0
TINY = 1e-30
SPLIT = 3


def step_kernel(
    dp,
    tp,
    table_hbm,
    lengths_hbm,
    counts_hbm,
    tokens_hbm,
    gain_hbm,
    check_hbm,
    wq_hbm,
    wk_hbm,
    wv_hbm,
    keys_hbm,
    values_hbm,
    out_ref,
    excess_ref,
    table_ref,
    lengths_ref,
    counts_ref,
    tokens_ref,
    gain_ref,
    check_ref,
    weights,
    keys,
    values,
    key_columns,
    weight_sums,
    check_row,
    outgoing,
    spread,
    parts,
    from_pair,
    outbound,
    from_chips,
    steps_out,
    steps_in,
    queries,
    new_keys,
    new_values,
    mixed,
    sums_all,
    sums_own,
    shares,
    excess_all,
    excess_own,
    small_sems,
    load_sems,
    a2a_send,
    a2a_recv,
    pair_send,
    pair_recv,
    chip_send,
    chip_recv,
    step_send,
    step_recv,
    sum_send,
    sum_recv,
    exc_send,
    exc_recv,
):
    chips = dp // 2
    spread_lanes = steps_out.shape[2]
    me = lax.axis_index("dp")
    zed = lax.axis_index("tensor")
    chip, core = me // 2, me % 2
    seqs, width = tokens_ref.shape
    depth = width // dp
    q_width, kv_width = wq_hbm.shape[1], wk_hbm.shape[1]
    total = q_width + 2 * kv_width
    chunks, _, _, chunk = parts.shape
    head = keys_hbm.shape[2]
    q_heads, kv_heads = q_width // head, kv_width // head
    group = q_heads // kv_heads
    pages = table_ref.shape[1]
    page_rows = keys_hbm.shape[1]

    def wait_bytes(ref, sem):
        pltpu.make_async_copy(ref, ref, sem).wait()

    def partner(dc):
        other, bit = chip, 1
        while bit <= dc:
            if dc // bit % 2:
                other = other + bit - 2 * bit * (chip // bit % 2)
            bit *= 2
        return other

    def slot(q, dc):
        return (1 - q if dc else q) * chips + dc

    barrier = pltpu.get_barrier_semaphore()
    for k in range(1, dp):
        pl.semaphore_signal(
            barrier, inc=1, device_id=((me + k) % dp, zed), device_id_type=MESH
        )

    small_loads = [
        pltpu.make_async_copy(source, target, small_sems.at[i])
        for i, (source, target) in enumerate(
            [
                (tokens_hbm, tokens_ref),
                (gain_hbm, gain_ref),
                (lengths_hbm, lengths_ref),
                (table_hbm, table_ref),
                (counts_hbm, counts_ref),
                (check_hbm, check_ref),
            ]
        )
    ]
    for load in small_loads:
        load.start()
    loads = [
        pltpu.make_async_copy(keys_hbm, keys, load_sems.at[1]),
        pltpu.make_async_copy(wq_hbm, weights.at[:, pl.ds(0, q_width)], load_sems.at[0]),
        pltpu.make_async_copy(wk_hbm, weights.at[:, pl.ds(q_width, kv_width)], load_sems.at[0]),
        pltpu.make_async_copy(
            wv_hbm, weights.at[:, pl.ds(q_width + kv_width, kv_width)], load_sems.at[0]
        ),
        pltpu.make_async_copy(values_hbm, values, load_sems.at[2]),
    ]

    loads[0].start()
    for load in small_loads[:2]:
        load.wait()
    for load in loads[1:4]:
        load.start()
    square = jnp.zeros((seqs, LANES), F32)
    for j in range(width // LANES):
        part = tokens_ref[:, j * LANES : (j + 1) * LANES].astype(F32)
        square = square + part * part
    scale = lax.rsqrt(jnp.sum(square, axis=1, keepdims=True) / width + EPSILON)
    gains = gain_ref[...].astype(F32)
    for j in range(width // LANES):
        part = tokens_ref[:, j * LANES : (j + 1) * LANES].astype(F32)
        at = j * LANES % depth
        outgoing[j * LANES // depth, :, at : at + LANES] = (
            part * scale * gains[j : j + 1]
        ).astype(BF16)
    spread[0] = outgoing[me]

    pl.semaphore_wait(barrier, dp - 1 + (zed + tp - 1) // tp)

    def greet_plane(k):
        @pl.when((zed + k >= 0) & (zed + k < tp))
        def _():
            pl.semaphore_signal(barrier, inc=1, device_id=(me, zed + k), device_id_type=MESH)


    for dc in range(chips - 1, -1, -1):
        for there in range(2) if dc else [1 - core]:
            q = (there + core) % 2
            target = partner(dc) * 2 + there
            copy = pltpu.make_async_remote_copy(
                src_ref=outgoing.at[target],
                dst_ref=spread.at[slot(q, dc)],
                send_sem=a2a_send,
                recv_sem=a2a_recv,
                device_id=(target, zed),
                device_id_type=MESH,
            )
            copy.start()

    greet_plane(1)
    for k in range(1, tp):
        greet_plane(-k)

    for load in small_loads[2:5]:
        load.wait()
    seq_row = lax.broadcasted_iota(jnp.int32, (seqs, LANES), 0)
    positions = jnp.zeros((seqs, LANES), F32)
    for s in range(seqs):
        positions = jnp.where(seq_row == s, lengths_ref[s].astype(F32), positions)
    lane = lax.broadcasted_iota(jnp.int32, (seqs, head), 1)
    step = (lane % (head // 2)).astype(F32)
    angles = positions * jnp.exp(step * (-2.0 * math.log(ROPE_BASE) / head))
    cosine = jnp.cos(angles)
    sine = jnp.where(lane < head // 2, -1.0, 1.0) * jnp.sin(angles)

    near = (pages + 1) // 2
    far = pages - near
    span = near * page_rows
    no_page = jnp.zeros((page_rows, head), BF16)

    def side_by_side(pool, s):
        left = [pool[table_ref[s, p]] for p in range(near)]
        right = [pool[table_ref[s, p]] for p in range(near, pages)] + [no_page] * (near - far)
        return jnp.concatenate(
            [jnp.concatenate(left, axis=0), jnp.concatenate(right, axis=0)], axis=1
        )

    def turn_keys(s, carry):
        key_columns[s] = jnp.transpose(side_by_side(keys, s))
        return carry

    loads[0].wait()
    loads[4].start()
    lax.fori_loop(0, seqs, turn_keys, 0, unroll=UNROLL)

    small_loads[5].wait()
    checks = check_ref[...].astype(F32)
    checked = jnp.zeros((seqs, LANES), F32)
    for j in range(width // LANES):
        at = j * LANES % depth
        part = outgoing[j * LANES // depth, :, at : at + LANES].astype(F32)
        checked = checked + part * checks[j : j + 1]
    shares[...] = jnp.zeros(shares.shape, F32)
    shares[me] = jnp.where(zed == 0, checked, 0.0)
    turned_checks = jnp.transpose(shares[...].reshape(dp * seqs, LANES))
    check_row[...] = jnp.sum(turned_checks, axis=0, keepdims=True)

    wait_bytes(weights, load_sems.at[0])

    totals = lax.dot_general(
        jnp.ones((seqs, total), BF16),
        weights[...],
        (((1,), (1,)), ((), ())),
        preferred_element_type=F32,
    )
    term = lax.broadcasted_iota(jnp.int32, (seqs, depth), 0)
    split = jnp.zeros((seqs, depth), F32)
    for i in range(SPLIT):
        rounded = totals.astype(BF16).astype(F32)
        split = jnp.where(term == i, rounded, split)
        totals = totals - rounded
    weight_sums[...] = split.astype(BF16)

    wait_bytes(spread.at[pl.ds(1, dp - 1)], a2a_recv)

    pair_copies = []
    middle = (chunks + 1) // 2
    step_groups = [(0, middle)] + [(middle, chunks)] * (chunks > 1)
    batch = seqs // 2
    half = chips * seqs

    def project(c):
        product = jnp.dot(
            spread[...].reshape(dp * seqs, depth),
            weights[:, pl.ds(c * chunk, chunk)],
            preferred_element_type=F32,
        )
        parts[c, 1] = product[half:]
        copy = pltpu.make_async_remote_copy(
            src_ref=parts.at[c, 1],
            dst_ref=from_pair.at[c],
            send_sem=pair_send,
            recv_sem=pair_recv.at[c],
            device_id=(chip * 2 + (core + 1) % 2, zed),
            device_id_type=MESH,
        )
        copy.start()
        pair_copies.append(copy)
        parts[c, 0] = product[:half]

    spots = lax.broadcasted_iota(jnp.int32, (half - seqs, spread_lanes), 1)
    spot_rows = lax.broadcasted_iota(jnp.int32, (half - seqs, spread_lanes), 0)

    def pass_on(c):
        pair_copies[c].wait_recv()
        summed = parts[c, 0, pl.ds(seqs, half - seqs)] + from_pair[c, pl.ds(seqs, half - seqs)]
        largest = jnp.max(jnp.abs(summed), axis=1, keepdims=True)
        step = (jnp.maximum(largest, TINY) * (1.0 / LEVELS)).astype(BF16).astype(F32)
        coded = jnp.round(summed * (1.0 / step)).astype(jnp.int32)
        for dc in range(1, chips):
            for h in range(2):
                at = (dc - 1) * seqs + h * batch
                stacked = jnp.concatenate(
                    [coded[at : at + batch, : chunk // 2], coded[at : at + batch, chunk // 2 :]],
                    axis=0,
                )
                outbound[h, c, dc - 1] = stacked.astype(jnp.int16)
        steps_out[c] = jnp.sum(jnp.where(spots == spot_rows, step, 0.0), axis=0, keepdims=True)
        for g, (first, last) in enumerate(step_groups):
            if c == last - 1:
                some = pl.ds(first, last - first)
                for dc in range(chips - 1, 0, -1):
                    send_on(
                        steps_out.at[some],
                        steps_in.at[dc - 1, some],
                        step_send,
                        step_recv.at[g],
                        dc,
                    )
        send_batch(0, c)

    def send_batch(h, c):
        for dc in range(chips - 1, 0, -1):
            send_on(
                outbound.at[h, c, dc - 1],
                from_chips.at[h, c, dc - 1],
                chip_send,
                chip_recv.at[c if h == 0 else chunks],
                dc,
            )

    def send_on(source, target, send_sem, recv_sem, dc):
        pltpu.make_async_remote_copy(
            src_ref=source,
            dst_ref=target,
            send_sem=send_sem,
            recv_sem=recv_sem,
            device_id=(partner(dc) * 2 + (core + 1) % 2, zed),
            device_id_type=MESH,
        ).start()

    def exchange(own, everyone, place, targets, send_sem, recv_sem):
        everyone[place] = own[...]
        for target in targets:
            pltpu.make_async_remote_copy(
                src_ref=own,
                dst_ref=everyone.at[place],
                send_sem=send_sem,
                recv_sem=recv_sem,
                device_id=target,
                device_id_type=MESH,
            ).start()

    def add_sums():
        blocks = []
        for owner in range(dp):
            there = owner // 2
            relative, bit = 0, 1
            while bit < chips:
                mine, other = chip // bit % 2, there // bit % 2
                relative = relative + bit * ((mine + other) % 2)
                bit *= 2
            kept = (core + owner + (relative + chips - 1) // chips) % 2
            blocks.append(spread[kept * chips + relative])
        terms = lax.dot_general(
            weight_sums[...],
            jnp.concatenate(blocks, axis=0),
            (((1,), (1,)), ((), ())),
            preferred_element_type=F32,
        )
        excess_own[...] = jnp.sum(terms, axis=0, keepdims=True) - check_row[...]

    def send_sums():
        exchange(
            excess_own, excess_all, me, [((me + k) % dp, zed) for k in range(1, dp)], exc_send, exc_recv
        )

    add_sums()
    for c in range(chunks):
        project(c)
        if c == 0:
            send_sums()
        if c >= 3:
            pass_on(c - 3)
    for c in range(max(chunks - 3, 0), chunks):
        pass_on(c)
    for c in range(chunks):
        send_batch(1, c)

    def finish_group():
        wait_bytes(excess_all.at[pl.ds(1, dp - 1)], exc_recv)
        group_sum = excess_all[0]
        for k in range(1, dp):
            group_sum = group_sum + excess_all[k]
        sums_own[...] = group_sum

        @pl.when(zed < tp - 1)
        def _():
            pl.semaphore_wait(barrier, tp - 1 - zed)

        exchange(
            sums_own, sums_all, zed, [(me, (zed + k) % tp) for k in range(1, tp)], sum_send, sum_recv
        )

    def rotate(vector, rows):
        return (
            (vector * cosine[rows] + pltpu.roll(vector, head // 2, 1) * sine[rows])
            .astype(BF16)
            .astype(F32)
        )

    def settle(h, c):
        if h == 0:
            for g, (first, last) in enumerate(step_groups):
                if c == first:
                    some = pl.ds(first, last - first)
                    wait_bytes(steps_in.at[:, some], step_recv.at[g])
            wait_bytes(from_chips.at[h, c], chip_recv.at[c])
        rows = slice(h * batch, (h + 1) * batch)
        own = parts[c, 0, rows] + from_pair[c, rows]
        for dc in range(1, chips):
            spot = spot_rows[rows] + (dc - 1) * seqs
            step = jnp.sum(
                jnp.where(spots[rows] == spot, steps_in[dc - 1, c], 0.0), axis=1, keepdims=True
            )
            stacked = from_chips[h, c, dc - 1].astype(jnp.int32).astype(F32)
            own = own + jnp.concatenate([stacked[:batch], stacked[batch:]], axis=1) * step
        for i in range(chunk // head):
            block = own[:, i * head : (i + 1) * head]
            index = c * (chunk // head) + i
            if index < q_heads:
                queries[rows, index, :] = rotate(block, rows)
            elif index < q_heads + kv_heads:
                k = index - q_heads
                turned = rotate(block, rows)
                for g in range(group):
                    new_keys[rows, k * group + g, :] = turned
            else:
                k = index - q_heads - kv_heads
                rounded = block.astype(BF16).astype(F32)
                for g in range(group):
                    new_values[rows, k * group + g, :] = rounded

    column = lax.broadcasted_iota(jnp.int32, (2 * q_heads, span), 1)
    row = lax.broadcasted_iota(jnp.int32, (2 * q_heads, span), 0)
    place = jnp.where(
        column % kv_heads == row % q_heads // group,
        column // kv_heads + row // q_heads * (span // kv_heads),
        pages * page_rows,
    )
    exponent_scale = head ** (-0.5) * math.log2(math.e)
    no_query = jnp.zeros((q_heads, head), BF16)
    loads[4].wait()

    def one_sequence(s):
        query = queries[s]
        narrow = query.astype(BF16)
        paired = jnp.concatenate(
            [
                jnp.concatenate([narrow, no_query], axis=1),
                jnp.concatenate([no_query, narrow], axis=1),
            ],
            axis=0,
        )
        scores = jnp.dot(paired, key_columns[s], preferred_element_type=F32)
        new_score = jnp.sum(query * new_keys[s], axis=1, keepdims=True)
        masked = jnp.where(place < lengths_ref[s], scores, -jnp.inf)
        highest = jnp.max(masked, axis=1, keepdims=True)
        peak = jnp.maximum(jnp.maximum(highest[:q_heads], highest[q_heads:]), new_score)
        soft = jnp.exp2((masked - jnp.concatenate([peak, peak], axis=0)) * exponent_scale)
        new_weight = jnp.exp2((new_score - peak) * exponent_scale)
        sums = jnp.sum(soft, axis=1, keepdims=True)
        denominator = sums[:q_heads] + sums[q_heads:] + new_weight
        result = jnp.dot(
            soft.astype(BF16), side_by_side(values, s), preferred_element_type=F32
        )
        result = result[:q_heads, :head] + result[q_heads:, head:]
        result = result + new_weight.astype(BF16).astype(F32) * new_values[s]
        mixed[s] = result / denominator

    for h in range(2):
        if h == 0:
            finish_group()
        else:
            wait_bytes(from_chips.at[1], chip_recv.at[chunks])
        for c in range(chunks):
            settle(h, c)
        for s in range(h * batch, (h + 1) * batch):
            one_sequence(s)
        rows = slice(h * batch, (h + 1) * batch)
        for i in range(q_heads):
            out_ref[rows, i * head : (i + 1) * head] = mixed[rows, i, :].astype(BF16)

    wait_bytes(sums_all.at[pl.ds(1, tp - 1)], sum_recv)
    grand = sums_all[0]
    for k in range(1, tp):
        grand = grand + sums_all[k]
    residual = grand / math.sqrt(total * tp)
    over = jnp.maximum(jnp.abs(residual) - TOL_STEP * counts_ref[...].astype(F32), 0.0)
    excess_ref[...] = jnp.broadcast_to(
        jnp.sum(over, axis=1, keepdims=True) / math.sqrt(seqs * dp), excess_ref.shape
    )

    wait_bytes(spread.at[pl.ds(1, dp - 1)], a2a_send)
    wait_bytes(from_pair, pair_send)
    wait_bytes(from_chips, chip_send)
    wait_bytes(steps_in, step_send)
    wait_bytes(sums_all.at[pl.ds(1, tp - 1)], sum_send)
    wait_bytes(excess_all.at[pl.ds(1, dp - 1)], exc_send)


def hand_out(attention, excess, attention_out, excess_out, single, sems):
    first = pltpu.make_async_copy(attention, attention_out, sems.at[0])
    first.start()
    single[...] = excess[0:1, 0:1]
    second = pltpu.make_async_copy(single, excess_out, sems.at[1])
    second.start()
    first.wait()
    second.wait()


def body(
    dp,
    tp,
    tokens,
    norm_gain,
    w_query,
    w_key,
    w_value,
    check_column,
    key_cache,
    value_cache,
    page_table,
    lengths,
    tol_counts,
):
    seqs, width = tokens.shape
    head = key_cache.shape[-1]
    q_width, kv_width = w_query.shape[1], w_key.shape[1]
    total = q_width + 2 * kv_width
    q_heads = q_width // head
    depth = width // dp
    chips = dp // 2
    chunks = 5 if total % (5 * head) == 0 else 1
    chunk = total // chunks
    spread_lanes = -(-(chips - 1) * seqs // LANES) * LANES
    flat_keys = key_cache.reshape(key_cache.shape[0], -1, head)
    flat_values = value_cache.reshape(value_cache.shape[0], -1, head)

    vmem = pl.BlockSpec(memory_space=pltpu.VMEM)
    hbm = pl.BlockSpec(memory_space=pltpu.HBM)
    dma = pltpu.SemaphoreType.DMA
    attention, excess = pl.pallas_call(
        functools.partial(step_kernel, dp, tp),
        out_shape=(
            pltpu.VMEM((seqs, q_width), BF16),
            pltpu.VMEM((8, LANES), F32),
        ),
        in_specs=[hbm] * 11,
        out_specs=(vmem, vmem),
        scratch_shapes=[
            pltpu.SMEM(page_table.shape, jnp.int32),
            pltpu.SMEM(lengths.shape, jnp.int32),
            pltpu.VMEM((1, tol_counts.shape[0]), jnp.int32),
            pltpu.VMEM(tokens.shape, BF16),
            pltpu.VMEM((width // LANES, LANES), BF16),
            pltpu.VMEM((width // LANES, LANES), BF16),
            pltpu.VMEM((depth, total), BF16),
            pltpu.VMEM(flat_keys.shape, BF16),
            pltpu.VMEM(flat_values.shape, BF16),
            pltpu.VMEM((seqs, 2 * head, (page_table.shape[1] + 1) // 2 * flat_keys.shape[1]), BF16),
            pltpu.VMEM((seqs, depth), BF16),
            pltpu.VMEM((1, dp * seqs), F32),
            pltpu.VMEM((dp, seqs, depth), BF16),
            pltpu.VMEM((dp, seqs, depth), BF16),
            pltpu.VMEM((chunks, 2, chips * seqs, chunk), F32),
            pltpu.VMEM((chunks, chips * seqs, chunk), F32),
            pltpu.VMEM((2, chunks, chips - 1, seqs, chunk // 2), jnp.int16),
            pltpu.VMEM((2, chunks, chips - 1, seqs, chunk // 2), jnp.int16),
            pltpu.VMEM((chunks, 1, spread_lanes), F32),
            pltpu.VMEM((chips - 1, chunks, 1, spread_lanes), F32),
            pltpu.VMEM((seqs, q_heads, head), F32),
            pltpu.VMEM((seqs, q_heads, head), F32),
            pltpu.VMEM((seqs, q_heads, head), F32),
            pltpu.VMEM((seqs, q_heads, head), F32),
            pltpu.VMEM((tp, 1, dp * seqs), F32),
            pltpu.VMEM((1, dp * seqs), F32),
            pltpu.VMEM((dp, seqs, LANES), F32),
            pltpu.VMEM((dp, 1, dp * seqs), F32),
            pltpu.VMEM((1, dp * seqs), F32),
            dma((6,)),
            dma((3,)),
            dma(()),
            dma(()),
            dma(()),
            dma((chunks,)),
            dma(()),
            dma((chunks + 1,)),
            dma(()),
            dma((2,)),
            dma(()),
            dma(()),
            dma(()),
            dma(()),
        ],
        compiler_params=pltpu.CompilerParams(
            collective_id=0, has_side_effects=True, vmem_limit_bytes=60 * 1024 * 1024
        ),
    )(
        page_table,
        lengths,
        tol_counts.reshape(1, -1),
        tokens,
        norm_gain.reshape(-1, LANES),
        check_column.reshape(-1, LANES),
        w_query,
        w_key,
        w_value,
        flat_keys,
        flat_values,
    )
    attention, excess = pl.pallas_call(
        hand_out,
        out_shape=(
            jax.ShapeDtypeStruct((seqs, q_width), BF16),
            jax.ShapeDtypeStruct((1, 1), F32),
        ),
        in_specs=[vmem, vmem],
        out_specs=(hbm, hbm),
        scratch_shapes=[pltpu.VMEM((1, 1), F32), dma((2,))],
    )(
        pltpu.with_memory_space_constraint(attention, pltpu.VMEM),
        pltpu.with_memory_space_constraint(excess, pltpu.VMEM),
    )
    return attention, excess[0, 0]


def solution(mesh):
    return jax.shard_map(
        functools.partial(body, mesh.shape["dp"], mesh.shape["tensor"]),
        mesh=mesh,
        in_specs=(
            P("dp", None),
            P(),
            P("dp", "tensor"),
            P("dp", "tensor"),
            P("dp", "tensor"),
            P(),
            P("dp", None, "tensor", None),
            P("dp", None, "tensor", None),
            P("dp", None),
            P("dp"),
            P(),
        ),
        out_specs=(P("dp", "tensor"), P()),
        check_vma=False,
    )
```
